32 devices in a mesh: wide: 8 (over y, x, core), narrow: 4 (over z).
Axes of the slice: x: 2, y: 2, z: 4, core: 2. Of those that a mesh axis runs over, the one named last changes fastest.
Arguments:
- tokens: bfloat16 [8192, 2048], P(('wide', 'narrow')), may hold values from -6 to 6
- out_grad: bfloat16 [8192, 2048], P(('wide', 'narrow')), may hold values from -6 to 6
- captions: bfloat16 [4096, 4096], P(('wide', 'narrow')), may hold values from -6 to 6
- image_blocks: int32 [32, 256], P('wide'), may hold values from 0 to 3, never falling along the last dimension, each value on 1 to 128 neighbouring positions
- caption_owner: int32 [8, 512], P('wide'), may hold values from 0 to 3, never falling along the last dimension, each value on 1 to 256 neighbouring positions
- norm_gains: float32 [3, 2048], replicated, may hold values from 0.25 to 1.75
- norm_shifts: float32 [3, 2048], replicated, may hold values from -3 to 3
- w_query: float32 [2048, 2048], P('wide', 'narrow'), may hold values from -0.125 to 0.125
- w_key: float32 [2048, 2048], P('wide', 'narrow'), may hold values from -0.125 to 0.125
- w_value: float32 [2048, 2048], P('wide', 'narrow'), may hold values from -0.125 to 0.125
- w_out: float32 [2048, 2048], P('narrow', 'wide'), may hold values from -0.375 to 0.375
- w_cross_query: float32 [2048, 2048], P('wide', 'narrow'), may hold values from -0.125 to 0.125
- w_cross_key: float32 [4096, 2048], P('wide', 'narrow'), may hold values from -0.09375 to 0.09375
- w_cross_value: float32 [4096, 2048], P('wide', 'narrow'), may hold values from -0.09375 to 0.09375
- w_cross_out: float32 [2048, 2048], P('narrow', 'wide'), may hold values from -0.375 to 0.375
- w_up: float32 [2048, 8192], P('wide', 'narrow'), may hold values from -0.125 to 0.125
- w_down: float32 [8192, 2048], P('narrow', 'wide'), may hold values from -0.0625 to 0.0625
Outputs:
- block_out: bfloat16 [8192, 2048], P(('wide', 'narrow'))
- grad_tokens: bfloat16 [8192, 2048], P(('wide', 'narrow'))
- grad_captions: bfloat16 [4096, 4096], P(('wide', 'narrow'))
- grad_norm_gains: float32 [3, 2048], replicated
- grad_norm_shifts: float32 [3, 2048], replicated
- grad_w_query: float32 [2048, 2048], P('wide', 'narrow')
- grad_w_key: float32 [2048, 2048], P('wide', 'narrow')
- grad_w_value: float32 [2048, 2048], P('wide', 'narrow')
- grad_w_out: float32 [2048, 2048], P('narrow', 'wide')
- grad_w_cross_query: float32 [2048, 2048], P('wide', 'narrow')
- grad_w_cross_key: float32 [4096, 2048], P('wide', 'narrow')
- grad_w_cross_value: float32 [4096, 2048], P('wide', 'narrow')
- grad_w_cross_out: float32 [2048, 2048], P('narrow', 'wide')
- grad_w_up: float32 [2048, 8192], P('wide', 'narrow')
- grad_w_down: float32 [8192, 2048], P('narrow', 'wide')
The draws below stay inside these ranges and needn't reach their ends.
Inputs may be any that keep to these rules, and one draw needn't show every extreme that they name: `image_blocks`: within an image the block numbers never fall; each of the 4 blocks has 1 to 128 tokens, and one block of every image has exactly that many. `caption_owner`: within a group the owners never fall; every image of the group has 1 to 256 caption tokens, and one image of every group has exactly 256.
All inputs are finite; a program needn't handle non-finite values.
Results may differ from the reference program's by a relative error of at most 0.024.
Values may be sent and summed in bfloat16 or wider, within the bound.
A program may use at most 320 MiB of HBM per device.

```python
import math
import jax
import jax.numpy as jnp
import numpy as np
from jax import lax

D = 2048
HEADS = 16
HEAD_DIM = 128
FF = 8192
TEXT_D = 4096
PIX = 256
BLOCKS = 4
CAP_DEV = 128
IMAGES = 32
TOKENS = 8192
CAP_GROUP = 512
CAPTIONS = 4096
N_WIDE = 8
N_NARROW = 4


def level_of(key, shape, split, low, largest):
    factor_of = 1.0
    for position, parts in split:
        steps = jax.random.uniform(jax.random.fold_in(jax.random.fold_in(key, 6), position), (parts,), jnp.float32, low / len(split), largest / len(split))
        factor_of = factor_of * jnp.repeat(jnp.exp(steps), shape[position] // parts).reshape((-1,) + (1,) * (len(shape) - 1 - position))
    return factor_of


def length_profile(count, total, most, slope):
    portions = [(1 << 20) // math.isqrt(standing ** slope) + 1 for standing in range(2, count + 1)]
    spare, given = total - most - (count - 1), [1] * (count - 1)
    while spare > 0:
        movable = [i for i in range(count - 1) if given[i] < most]
        whole, remaining = sum([portions[i] for i in movable]), spare
        for i in movable:
            more = min(most - given[i], max(1, remaining * portions[i] // whole), spare)
            given[i] = given[i] + more
            spare = spare - more
    return np.array([most] + given)


def ragged_sizes(rng, number_of, total, limit, slope):
    if number_of == 2:
        one = jax.random.randint(rng, (), max(1, total - limit), min(limit, total - 1) + 1)
        return jnp.stack([one, total - one])
    lengths = jnp.asarray(length_profile(number_of, total, limit, slope), jnp.int32)
    twos = (number_of - 1) // 2
    giver, sink = lengths[1:1 + 2 * twos:2], lengths[2:2 + 2 * twos:2]
    slack = jnp.minimum(giver - 1, limit - sink)
    shifted = jax.random.randint(jax.random.fold_in(rng, 1), (twos,), 0, 1 << 20) % (slack + 1)
    lengths = lengths.at[1:1 + 2 * twos:2].set(giver - shifted).at[2:2 + 2 * twos:2].set(sink + shifted)
    return lengths[jax.random.permutation(jax.random.fold_in(rng, 2), number_of)]


def scatter_about(own_key, extent, scale, bound, cuts=(), kind=jnp.bfloat16):
    result = jax.random.normal(own_key, extent, jnp.float32) * scale
    if len(cuts) > 0:
        result = level_of(own_key, extent, cuts, -0.22, 0.18) * result
    return jnp.clip(result, min=-bound, max=bound).astype(kind)


def setup_inputs(seed: int = 0) -> dict:
    keys = jax.random.split(jax.random.key(seed), 18)
    return {
        "tokens": scatter_about(keys[0], (TOKENS, D), 1.0, 6.0, ((0, 32),)),
        "out_grad": scatter_about(keys[1], (TOKENS, D), 1.0, 6.0, ((0, 32),)),
        "captions": scatter_about(keys[2], (CAPTIONS, TEXT_D), 1.0, 6.0, ((0, 32),)),
        "image_blocks": jax.vmap(lambda own: jnp.searchsorted(jnp.cumsum(ragged_sizes(own, BLOCKS, PIX, PIX // 2, 0)), jnp.arange(PIX), side="right"))(jax.random.split(keys[3], IMAGES)).reshape((IMAGES, PIX)).astype(jnp.int32),
        "caption_owner": jax.vmap(lambda own: jnp.searchsorted(jnp.cumsum(ragged_sizes(own, N_NARROW, CAP_GROUP, 2 * CAP_DEV, 1)), jnp.arange(CAP_GROUP), side="right"))(jax.random.split(keys[4], N_WIDE)).reshape((N_WIDE, CAP_GROUP)).astype(jnp.int32),
        "norm_gains": jnp.clip(1.0 + 0.15 * jax.random.normal(keys[5], (3, D), jnp.float32), 0.25, 1.75),
        "norm_shifts": scatter_about(keys[6], (3, D), 0.3, 3.0, (), jnp.float32),
        "w_query": scatter_about(keys[7], (D, D), D ** -0.5, 0.125, ((0, 8), (1, 4)), jnp.float32),
        "w_key": scatter_about(keys[8], (D, D), D ** -0.5, 0.125, ((0, 8), (1, 4)), jnp.float32),
        "w_value": scatter_about(keys[9], (D, D), D ** -0.5, 0.125, ((0, 8), (1, 4)), jnp.float32),
        "w_out": scatter_about(keys[10], (D, D), (D // 8) ** -0.5, 0.375, ((0, 4), (1, 8)), jnp.float32),
        "w_cross_query": scatter_about(keys[11], (D, D), D ** -0.5, 0.125, ((0, 8), (1, 4)), jnp.float32),
        "w_cross_key": scatter_about(keys[12], (TEXT_D, D), TEXT_D ** -0.5, 0.09375, ((0, 8), (1, 4)), jnp.float32),
        "w_cross_value": scatter_about(keys[13], (TEXT_D, D), TEXT_D ** -0.5, 0.09375, ((0, 8), (1, 4)), jnp.float32),
        "w_cross_out": scatter_about(keys[14], (D, D), (D // 8) ** -0.5, 0.375, ((0, 4), (1, 8)), jnp.float32),
        "w_up": scatter_about(keys[15], (D, FF), D ** -0.5, 0.125, ((0, 8), (1, 4)), jnp.float32),
        "w_down": scatter_about(keys[16], (FF, D), FF ** -0.5, 0.0625, ((0, 4), (1, 8)), jnp.float32),
    }


@jax.custom_vjp
def low(v):
    return lax.optimization_barrier(v.astype(jnp.bfloat16)).astype(jnp.float32)

@jax.custom_vjp
def low_back(v):
    return v

def low_keep(v):
    return (low(v), None)

def lower_precision_forward(kept, grad):
    return (grad,)

def back_keep(v):
    return (v, None)

def back_low(kept, grad):
    return (low(grad),)
low.defvjp(low_keep, lower_precision_forward)
low_back.defvjp(back_keep, back_low)
EPSILON = 1e-06
MASKED = -1000000000.0
HIGHEST_PRECISION = lax.Precision.HIGHEST

def norm_apply(features, norm_gain, norm_shift):
    center = features - lax.optimization_barrier(jnp.mean(features, axis=-1, keepdims=True))
    spread = lax.optimization_barrier(jnp.mean(center * center, axis=-1, keepdims=True))
    return center * lax.rsqrt(spread + EPSILON) * norm_gain + norm_shift

def product(left_side, right_side):
    return jnp.dot(left_side, right_side, precision=HIGHEST_PRECISION, preferred_element_type=jnp.float32)

def attend(queries, keys_in, values_in, allowed, score_scale):
    raw_scores = low_back(jnp.einsum('iphe,iqhe->ihpq', queries, keys_in, precision=HIGHEST_PRECISION)) * score_scale
    scores = jnp.where(allowed[:, None], raw_scores, MASKED)
    log_total = jax.nn.logsumexp(scores, axis=-1, keepdims=True)
    soft_weights = low(jnp.exp(scores - log_total))
    return jnp.einsum('ihpq,iqhe->iphe', soft_weights, values_in, precision=HIGHEST_PRECISION)

def self_group(pieces):
    queries, keys_in, values_in, blocks_here = pieces
    head_shape = (N_NARROW, PIX, HEADS, HEAD_DIM)
    allowed = blocks_here[:, :, None] == blocks_here[:, None, :]
    mixture = attend(queries.reshape(head_shape), keys_in.reshape(head_shape), values_in.reshape(head_shape), allowed, HEAD_DIM ** (-0.5))
    return mixture.reshape(N_NARROW * PIX, D)

def cross_group(pieces):
    queries, keys_in, values_in, owners = pieces
    row_count = N_NARROW * PIX
    image_of = jnp.arange(row_count, dtype=jnp.int32) // PIX
    allowed = (image_of[:, None] == owners[None, :])[None]
    mixture = attend(queries.reshape(1, row_count, HEADS, HEAD_DIM), keys_in.reshape(1, CAP_GROUP, HEADS, HEAD_DIM), values_in.reshape(1, CAP_GROUP, HEADS, HEAD_DIM), allowed, HEAD_DIM ** (-0.5))
    return mixture.reshape(row_count, D)

def block_forward(token_rows, caption_rows, norm_gains, norm_shifts, w_query, w_key, w_value, w_out, w_cross_query, w_cross_key, w_cross_value, w_cross_out, w_up, w_down, image_blocks, caption_owner):
    group_rows = N_NARROW * PIX

    def grouped(flat_rows):
        return flat_rows.reshape(N_WIDE, group_rows, flat_rows.shape[-1])
    first_normalized = low(norm_apply(token_rows, norm_gains[0], norm_shifts[0]))
    self_query = low(low_back(product(first_normalized, low(w_query))))
    self_keys = low(low_back(product(first_normalized, low(w_key))))
    self_values = low(low_back(product(first_normalized, low(w_value))))
    self_mix = lax.map(jax.checkpoint(self_group), (grouped(self_query), grouped(self_keys), grouped(self_values), image_blocks.reshape(N_WIDE, N_NARROW, PIX)))
    self_mix = low(low_back(self_mix.reshape(TOKENS, D)))
    residual1 = token_rows + low_back(product(self_mix, low(w_out)))
    normed2 = low(norm_apply(residual1, norm_gains[1], norm_shifts[1]))
    cross_query = low(low_back(product(normed2, low(w_cross_query))))
    cross_keys = low(low_back(product(caption_rows, low(w_cross_key))))
    cross_values = low(low_back(product(caption_rows, low(w_cross_value))))
    cross_mix = lax.map(jax.checkpoint(cross_group), (grouped(cross_query), cross_keys.reshape(N_WIDE, CAP_GROUP, D), cross_values.reshape(N_WIDE, CAP_GROUP, D), caption_owner))
    cross_mix = low(low_back(cross_mix.reshape(TOKENS, D)))
    residual2 = residual1 + low_back(product(cross_mix, low(w_cross_out)))
    normed3 = low(norm_apply(residual2, norm_gains[2], norm_shifts[2]))
    hidden = low_back(product(normed3, low(w_up)))
    acted = low(jax.nn.gelu(hidden))
    return residual2 + low_back(product(acted, low(w_down)))

def reference(tokens, out_grad, captions, image_blocks, caption_owner, norm_gains, norm_shifts, w_query, w_key, w_value, w_out, w_cross_query, w_cross_key, w_cross_value, w_cross_out, w_up, w_down):

    def forward(token_rows, caption_rows, gains, shifts, wq_master, wk_master, wv_master, wo_master, cq_master, ck_master, cv_master, co_master, up_master, down_master):
        return block_forward(token_rows, caption_rows, gains, shifts, wq_master, wk_master, wv_master, wo_master, cq_master, ck_master, cv_master, co_master, up_master, down_master, image_blocks, caption_owner)
    block_out, pullback = jax.vjp(forward, tokens.astype(jnp.float32), captions.astype(jnp.float32), norm_gains, norm_shifts, w_query, w_key, w_value, w_out, w_cross_query, w_cross_key, w_cross_value, w_cross_out, w_up, w_down)
    grads = pullback(out_grad.astype(jnp.float32))
    return (block_out.astype(jnp.bfloat16), grads[0].astype(jnp.bfloat16), grads[1].astype(jnp.bfloat16), grads[2], grads[3], grads[4], grads[5], grads[6], grads[7], grads[8], grads[9], grads[10], grads[11], grads[12], grads[13])
```

```python
import jax
import jax.numpy as jnp
from jax import lax
from jax.sharding import PartitionSpec as P

HEAD_DIM = 128
PIX = 256
CHUNKS = 2

EPSILON = 1e-06
MASKED = -1000000000.0
BF = jnp.bfloat16
F32 = jnp.float32


def product(left_side, right_side):
    return lax.dot_general(
        left_side,
        right_side,
        (((left_side.ndim - 1,), (0,)), ((), ())),
        preferred_element_type=F32,
    )


def right_inner(left_side, right_side):
    return lax.dot_general(
        left_side,
        right_side,
        (((left_side.ndim - 1,), (1,)), ((), ())),
        preferred_element_type=F32,
    )


def left_inner(left_side, right_side):
    rows = tuple(range(left_side.ndim - 1))
    return lax.dot_general(left_side, right_side, ((rows, rows), ((), ())), preferred_element_type=F32)


def spread(rows):
    n = lax.axis_size("narrow")
    here = lax.axis_index("narrow")
    up, down = [rows], [rows]
    for step in range(1, n):
        up.append(lax.ppermute(up[-1], "narrow", [(k, k + 1) for k in range(step - 1, n - 1)]))
        down.append(lax.ppermute(down[-1], "narrow", [(k, k - 1) for k in range(1, n - step + 1)]))
    parts = [rows] + [jnp.where(here >= s, up[s], down[n - s]) for s in range(1, n)]
    return jnp.stack(parts)


def sink(parts):
    n = lax.axis_size("narrow")
    up = down = None
    for step in range(1, n):
        one, other = parts[step], parts[n - step]
        if up is not None:
            one = up.astype(F32) + one.astype(F32)
            other = down.astype(F32) + other.astype(F32)
        up = lax.ppermute(one.astype(BF), "narrow", [(k, k + 1) for k in range(step)])
        down = lax.ppermute(other.astype(BF), "narrow", [(k, k - 1) for k in range(n - step, n)])
    return up.astype(F32) + down.astype(F32) + parts[0].astype(F32)


def norm_stats(features):
    center = features - jnp.mean(features, axis=-1, keepdims=True)
    rstd = lax.rsqrt(jnp.mean(center * center, axis=-1, keepdims=True) + EPSILON)
    return center * rstd, rstd


def norm_back(grad, xhat, rstd, gain):
    scaled = grad * gain
    return rstd * (
        scaled
        - jnp.mean(scaled, axis=-1, keepdims=True)
        - xhat * jnp.mean(scaled * xhat, axis=-1, keepdims=True)
    )


def norm_sums(grad, xhat):
    return jnp.stack([jnp.sum(grad * xhat, axis=0), jnp.sum(grad, axis=0)])


def score_block(queries, keys_in, allowed, score_scale):
    raw = jnp.einsum("iphe,iqhe->ihpq", queries, keys_in, preferred_element_type=F32)
    return jnp.where(allowed[:, None], raw * score_scale, MASKED)


def attend(queries, keys_in, values_in, allowed, score_scale):
    scores = score_block(queries, keys_in, allowed, score_scale)
    log_total = jax.nn.logsumexp(scores, axis=-1, keepdims=True)
    soft = jnp.exp(scores - log_total).astype(BF)
    mixture = jnp.einsum("ihpq,iqhe->iphe", soft, values_in, preferred_element_type=F32)
    return mixture.astype(BF), log_total


def attend_back(queries, keys_in, values_in, allowed, log_total, grad_mix, score_scale):
    soft = jnp.exp(score_block(queries, keys_in, allowed, score_scale) - log_total)
    grad_soft = jnp.einsum("iphe,iqhe->ihpq", grad_mix, values_in, preferred_element_type=F32)
    grad_values = jnp.einsum("ihpq,iphe->iqhe", soft.astype(BF), grad_mix, preferred_element_type=F32)
    row_dot = jnp.sum(soft * grad_soft, axis=-1, keepdims=True)
    grad_scores = (soft * (grad_soft - row_dot) * score_scale).astype(BF)
    grad_queries = jnp.einsum("ihpq,iqhe->iphe", grad_scores, keys_in, preferred_element_type=F32)
    grad_keys = jnp.einsum("ihpq,iphe->iqhe", grad_scores, queries, preferred_element_type=F32)
    return grad_queries.astype(BF), grad_keys, grad_values


def after(value, *others):
    return lax.optimization_barrier((value, *others))[0]


def body(
    tokens,
    out_grad,
    captions,
    image_blocks,
    caption_owner,
    norm_gains,
    norm_shifts,
    w_query,
    w_key,
    w_value,
    w_out,
    w_cross_query,
    w_cross_key,
    w_cross_value,
    w_cross_out,
    w_up,
    w_down,
):
    scale = HEAD_DIM ** (-0.5)
    n = lax.axis_size("narrow")
    here = lax.axis_index("narrow")
    width = w_query.shape[1]
    heads = width // HEAD_DIM
    part = PIX // CHUNKS
    chunks = [slice(c * part, (c + 1) * part) for c in range(CHUNKS)]
    image_of = (here - jnp.arange(n)) % n

    def rows_of(*pieces):
        return lax.all_gather(
            jnp.concatenate([p.astype(BF) for p in pieces], axis=1), "wide", axis=0, tiled=True
        )

    def columns_of(piece):
        return lax.all_gather(piece.astype(BF), "wide", axis=1, tiled=True)

    def to_rows(g):
        return lax.psum_scatter(g.astype(BF), "wide", scatter_dimension=0, tiled=True).astype(F32)

    def to_columns(g):
        return lax.psum_scatter(g.astype(BF), "wide", scatter_dimension=1, tiled=True).astype(F32)

    full_qkv = rows_of(w_query, w_key, w_value)
    full_out = columns_of(w_out)
    full_ckv = rows_of(w_cross_key, w_cross_value)
    full_cq = rows_of(w_cross_query)
    full_cout = columns_of(w_cross_out)
    full_up = rows_of(w_up)
    full_down = columns_of(w_down)

    residual0 = tokens.astype(F32)
    xhat1, rstd1 = norm_stats(residual0)
    own1 = (xhat1 * norm_gains[0] + norm_shifts[0]).astype(BF)
    normed1 = spread(own1)
    qkv = product(normed1, full_qkv).astype(BF)
    heads_of = lambda x: x.reshape(x.shape[:-1] + (x.shape[-1] // HEAD_DIM, HEAD_DIM))
    self_q, self_k, self_v = [heads_of(qkv[..., k * width : (k + 1) * width]) for k in range(3)]
    blocks = image_blocks[image_of]
    self_allowed = blocks[:, :, None] == blocks[:, None, :]
    self_mix, self_total = attend(self_q, self_k, self_v, self_allowed, scale)
    self_mix = self_mix.reshape(n, PIX, width)

    text = spread(after(captions, normed1))
    text_count = text.shape[0] * text.shape[1]
    text_rows = text.reshape(text_count, text.shape[2])
    ckv = product(text_rows, full_ckv).astype(BF)
    cross_k = heads_of(ckv[None, :, :width])
    cross_v = heads_of(ckv[None, :, width:])
    owner = caption_owner[0].reshape(n, -1)[image_of].reshape(-1)
    part_image = jnp.repeat(image_of, part)
    cross_allowed = (part_image[:, None] == owner[None, :])[None]

    state = []
    for rows in chunks:
        residual1 = residual0[rows] + sink(product(self_mix[:, rows], full_out).astype(BF))
        xhat2, rstd2 = norm_stats(residual1)
        state.append((residual1, xhat2, rstd2))
    normed2 = [spread((s[1] * norm_gains[1] + norm_shifts[1]).astype(BF)) for s in state]
    grad_all = spread(after(out_grad, normed2[0]))

    cross_q, cross_mix, cross_total, state3 = [], [], [], []
    for c in range(CHUNKS):
        q = heads_of(product(normed2[c], full_cq).astype(BF).reshape(1, n * part, width))
        mix, total = attend(q, cross_k, cross_v, cross_allowed, scale)
        mix = mix.reshape(n, part, width)
        residual2 = state[c][0] + sink(product(mix, full_cout).astype(BF))
        xhat3, rstd3 = norm_stats(residual2)
        cross_q.append(q)
        cross_mix.append(mix)
        cross_total.append(total)
        state3.append((residual2, xhat3, rstd3))
    normed3 = [spread((s[1] * norm_gains[2] + norm_shifts[2]).astype(BF)) for s in state3]

    block_out, acts, grad_hiddens, grad2, sums3 = [], [], [], [], []
    for c, rows in enumerate(chunks):
        hidden = product(normed3[c], full_up)
        grad_rows = grad_all[:, rows]
        acted, gelu_back = jax.vjp(jax.nn.gelu, hidden)
        acted = acted.astype(BF)
        grad_hidden = gelu_back(right_inner(grad_rows, full_down))[0].astype(BF)
        acts.append(acted)
        grad_hiddens.append(grad_hidden)
        grad_n3 = sink(right_inner(grad_hidden, full_up).astype(BF))
        residual2, xhat3, rstd3 = state3[c]
        sums3.append(norm_sums(grad_n3, xhat3))
        grad2.append(out_grad[rows].astype(F32) + norm_back(grad_n3, xhat3, rstd3, norm_gains[2]))
        block_out.append(
            (residual2 + sink(product(acted, full_down).astype(BF))).astype(BF)
        )
    cat = lambda xs: jnp.concatenate(xs, axis=1)
    acted, grad_hidden, n3 = cat(acts), cat(grad_hiddens), cat(normed3)
    grad_down = left_inner(acted, cat([grad_all[:, rows] for rows in chunks]))
    grad_up = left_inner(n3, grad_hidden)

    e2 = [spread(g.astype(BF)) for g in grad2]
    own_down = to_columns(grad_down)
    own_up = to_rows(grad_up)
    e2[-1] = after(e2[-1], grad_down, grad_up)
    grad1, sums2, grad_cqs, grad_ck, grad_cv = [], [], [], 0.0, 0.0
    for c in range(CHUNKS):
        grad_mix = heads_of(right_inner(e2[c], full_cout).astype(BF).reshape(1, n * part, width))
        gq, gk, gv = attend_back(
            cross_q[c], cross_k, cross_v, cross_allowed, cross_total[c], grad_mix, scale
        )
        gq = gq.reshape(n, part, width)
        grad_cqs.append(gq)
        grad_ck = grad_ck + gk
        grad_cv = grad_cv + gv
        grad_n2 = sink(right_inner(gq, full_cq).astype(BF))
        _, xhat2, rstd2 = state[c]
        sums2.append(norm_sums(grad_n2, xhat2))
        grad1.append(grad2[c] + norm_back(grad_n2, xhat2, rstd2, norm_gains[1]))
    grad_cout = left_inner(cat(cross_mix), cat(e2))
    grad_cq = left_inner(cat(normed2), cat(grad_cqs))
    grad_ckv = jnp.concatenate(
        [grad_ck.reshape(text_count, width), grad_cv.reshape(text_count, width)], axis=1
    ).astype(BF)
    grad_text_part = right_inner(grad_ckv, full_ckv).astype(BF).reshape(n, -1, text.shape[2])
    grad_wckv = left_inner(text_rows, grad_ckv)

    e1 = [spread(g.astype(BF)) for g in grad1]
    own_cout = to_columns(grad_cout)
    own_cq = to_rows(grad_cq)
    own_ckv = to_rows(grad_wckv)
    e1[-1] = after(e1[-1], grad_cout, grad_cq, grad_wckv, grad_text_part)
    grad_mix = heads_of(cat([right_inner(e, full_out).astype(BF) for e in e1]))
    grad_mix = after(grad_mix, own_down, own_up)
    gq, gk, gv = attend_back(self_q, self_k, self_v, self_allowed, self_total, grad_mix, scale)
    grad_qkv = jnp.concatenate(
        [g.astype(BF).reshape(n, PIX, width) for g in (gq, gk, gv)], axis=-1
    )
    grad_out = left_inner(self_mix, cat(e1))
    grad_wqkv = left_inner(normed1, grad_qkv)
    grad_n1 = sink(right_inner(after(grad_qkv, grad_wqkv), full_qkv).astype(BF))
    grad_text = sink(after(grad_text_part, grad_mix)).astype(BF)
    grad1 = jnp.concatenate(grad1)
    grad_n1 = after(grad_n1, own_cout, own_cq, own_ckv)
    grad_tokens = (grad1 + norm_back(grad_n1, xhat1, rstd1, norm_gains[0])).astype(BF)
    sums = lax.psum(
        jnp.stack([norm_sums(grad_n1, xhat1), sum(sums2), sum(sums3)]), ("wide", "narrow")
    )

    own_out = to_columns(grad_out)
    own_qkv = to_rows(grad_wqkv)
    return (
        jnp.concatenate(block_out),
        grad_tokens,
        grad_text,
        sums[:, 0],
        sums[:, 1],
        own_qkv[:, :width],
        own_qkv[:, width : 2 * width],
        own_qkv[:, 2 * width :],
        own_out,
        own_cq,
        own_ckv[:, :width],
        own_ckv[:, width:],
        own_cout,
        own_up,
        own_down,
    )

def solution(mesh):
    in_specs = (
        P(("wide", "narrow"), None),
        P(("wide", "narrow"), None),
        P(("wide", "narrow"), None),
        P("wide", None),
        P("wide", None),
        P(),
        P(),
        P("wide", "narrow"),
        P("wide", "narrow"),
        P("wide", "narrow"),
        P("narrow", "wide"),
        P("wide", "narrow"),
        P("wide", "narrow"),
        P("wide", "narrow"),
        P("narrow", "wide"),
        P("wide", "narrow"),
        P("narrow", "wide"),
    )
    out_specs = (
        P(("wide", "narrow"), None),
        P(("wide", "narrow"), None),
        P(("wide", "narrow"), None),
        P(),
        P(),
        P("wide", "narrow"),
        P("wide", "narrow"),
        P("wide", "narrow"),
        P("narrow", "wide"),
        P("wide", "narrow"),
        P("wide", "narrow"),
        P("wide", "narrow"),
        P("narrow", "wide"),
        P("wide", "narrow"),
        P("narrow", "wide"),
    )
    return jax.shard_map(body, mesh=mesh, in_specs=in_specs, out_specs=out_specs, check_vma=False)
```

```python
import jax
import jax.numpy as jnp
from jax import lax
from jax.sharding import PartitionSpec as P

HEAD_DIM = 128
PIX = 256
CHUNKS = 2

EPSILON = 1e-06
MASKED = -1000000000.0
BF = jnp.bfloat16
F32 = jnp.float32


def product(left_side, right_side):
    return lax.dot_general(
        left_side,
        right_side,
        (((left_side.ndim - 1,), (0,)), ((), ())),
        preferred_element_type=F32,
    )


def right_inner(left_side, right_side):
    return lax.dot_general(
        left_side,
        right_side,
        (((left_side.ndim - 1,), (1,)), ((), ())),
        preferred_element_type=F32,
    )


def left_inner(left_side, right_side):
    rows = tuple(range(left_side.ndim - 1))
    return lax.dot_general(left_side, right_side, ((rows, rows), ((), ())), preferred_element_type=F32)


def after(value, *others):
    if not others:
        return value
    nothing = sum(o[(0,) * o.ndim].astype(F32) for o in others) * 0.0
    return value + nothing.astype(value.dtype)


def whole(value):
    return lax.optimization_barrier(value)


def spread(name, rows, gates={}):
    n = lax.axis_size("narrow")
    here = lax.axis_index("narrow")
    with jax.named_scope("spread_" + name):
        up, down = [rows], [rows]
        for step in range(1, n):
            one, other = after(up[-1], *gates.get(step, ())), after(down[-1], *gates.get(step, ()))
            up.append(lax.ppermute(one, "narrow", [(k, k + 1) for k in range(step - 1, n - 1)]))
            down.append(lax.ppermute(other, "narrow", [(k, k - 1) for k in range(1, n - step + 1)]))
        parts = [rows] + [jnp.where(here >= s, up[s], down[n - s]) for s in range(1, n)]
        return jnp.stack(parts), [(up[s], down[s]) for s in range(1, n)]


def sink(name, parts, gates={}):
    n = lax.axis_size("narrow")
    hops = []
    with jax.named_scope("sink_" + name):
        for step in range(1, n):
            one, other = parts[step], parts[n - step]
            gate = gates.get(step, ())
            if callable(gate):
                gate = gate(hops[0])
            if hops:
                one = hops[-1][0].astype(F32) + one.astype(F32)
                other = hops[-1][1].astype(F32) + other.astype(F32)
            one, other = after(one, *gate), after(other, *gate)
            up = lax.ppermute(one.astype(BF), "narrow", [(k, k + 1) for k in range(step)])
            down = lax.ppermute(other.astype(BF), "narrow", [(k, k - 1) for k in range(n - step, n)])
            hops.append((up, down))
        return up.astype(F32) + down.astype(F32) + parts[0].astype(F32), hops


def norm_stats(features):
    center = features - jnp.mean(features, axis=-1, keepdims=True)
    rstd = lax.rsqrt(jnp.mean(center * center, axis=-1, keepdims=True) + EPSILON)
    return center * rstd, rstd


def norm_back(grad, xhat, rstd, gain):
    scaled = grad * gain
    return rstd * (
        scaled
        - jnp.mean(scaled, axis=-1, keepdims=True)
        - xhat * jnp.mean(scaled * xhat, axis=-1, keepdims=True)
    )


def norm_sums(grad, xhat):
    return jnp.stack([jnp.sum(grad * xhat, axis=0), jnp.sum(grad, axis=0)])


def score_block(queries, keys_in, allowed, score_scale):
    raw = jnp.einsum("iphe,iqhe->ihpq", queries, keys_in, preferred_element_type=F32)
    return jnp.where(allowed[:, None], raw * score_scale, MASKED)


def attend(queries, keys_in, values_in, allowed, score_scale):
    scores = score_block(queries, keys_in, allowed, score_scale)
    log_total = jax.nn.logsumexp(scores, axis=-1, keepdims=True)
    soft = jnp.exp(scores - log_total).astype(BF)
    mixture = jnp.einsum("ihpq,iqhe->iphe", soft, values_in, preferred_element_type=F32)
    return mixture.astype(BF), log_total


def attend_back(queries, keys_in, values_in, allowed, log_total, grad_mix, score_scale):
    soft = jnp.exp(score_block(queries, keys_in, allowed, score_scale) - log_total)
    grad_soft = jnp.einsum("iphe,iqhe->ihpq", grad_mix, values_in, preferred_element_type=F32)
    grad_values = jnp.einsum("ihpq,iphe->iqhe", soft.astype(BF), grad_mix, preferred_element_type=F32)
    row_dot = jnp.sum(soft * grad_soft, axis=-1, keepdims=True)
    grad_scores = (soft * (grad_soft - row_dot) * score_scale).astype(BF)
    grad_queries = jnp.einsum("ihpq,iqhe->iphe", grad_scores, keys_in, preferred_element_type=F32)
    grad_keys = jnp.einsum("ihpq,iphe->iqhe", grad_scores, queries, preferred_element_type=F32)
    return grad_queries.astype(BF), grad_keys, grad_values


def body(
    tokens,
    out_grad,
    captions,
    image_blocks,
    caption_owner,
    norm_gains,
    norm_shifts,
    w_query,
    w_key,
    w_value,
    w_out,
    w_cross_query,
    w_cross_key,
    w_cross_value,
    w_cross_out,
    w_up,
    w_down,
):
    scale = HEAD_DIM ** (-0.5)
    n = lax.axis_size("narrow")
    here = lax.axis_index("narrow")
    width = w_query.shape[1]
    heads = width // HEAD_DIM
    part = PIX // CHUNKS
    chunks = [slice(c * part, (c + 1) * part) for c in range(CHUNKS)]
    image_of = (here - jnp.arange(n)) % n

    def rows_of(*pieces):
        return lax.all_gather(
            jnp.concatenate([p.astype(BF) for p in pieces], axis=1), "wide", axis=0, tiled=True
        )

    def columns_of(piece):
        return lax.all_gather(piece.astype(BF), "wide", axis=1, tiled=True)

    def to_rows(g):
        return lax.psum_scatter(g.astype(BF), "wide", scatter_dimension=0, tiled=True).astype(F32)

    def to_columns(g):
        return lax.psum_scatter(g.astype(BF), "wide", scatter_dimension=1, tiled=True).astype(F32)

    full_qkv = rows_of(w_query, w_key, w_value)
    full_out = columns_of(w_out)
    full_ckv = rows_of(w_cross_key, w_cross_value)
    full_cq = rows_of(w_cross_query)
    full_cout = columns_of(w_cross_out)
    full_up = rows_of(w_up)
    full_down = columns_of(w_down)

    residual0 = tokens.astype(F32)
    xhat1, rstd1 = norm_stats(residual0)
    own1 = (xhat1 * norm_gains[0] + norm_shifts[0]).astype(BF)
    normed1 = spread("n1", own1)[0]
    qkv = product(normed1, full_qkv).astype(BF)
    heads_of = lambda x: x.reshape(x.shape[:-1] + (x.shape[-1] // HEAD_DIM, HEAD_DIM))
    self_q, self_k, self_v = [heads_of(qkv[..., k * width : (k + 1) * width]) for k in range(3)]
    blocks = image_blocks[image_of]
    self_allowed = blocks[:, :, None] == blocks[:, None, :]
    self_mix, self_total = attend(self_q, self_k, self_v, self_allowed, scale)
    self_mix = self_mix.reshape(n, PIX, width)

    text = spread("text", after(captions, normed1[1], normed1[n - 1]), {2: (self_mix,)})[0]
    text_count = text.shape[0] * text.shape[1]
    text_rows = text.reshape(text_count, text.shape[2])
    ckv = product(text_rows, full_ckv).astype(BF)
    cross_k = heads_of(ckv[None, :, :width])
    cross_v = heads_of(ckv[None, :, width:])
    owner = caption_owner[0].reshape(n, -1)[image_of].reshape(-1)
    part_image = jnp.repeat(image_of, part)
    cross_allowed = (part_image[:, None] == owner[None, :])[None]

    state = []
    for c, rows in enumerate(chunks):
        residual1 = residual0[rows] + sink(f"r1_{c}", product(self_mix[:, rows], full_out).astype(BF))[0]
        xhat2, rstd2 = norm_stats(residual1)
        state.append((residual1, xhat2, rstd2))
    normed2 = [
        spread(f"n2_{c}", (s[1] * norm_gains[1] + norm_shifts[1]).astype(BF))[0] for c, s in enumerate(state)
    ]
    grad_all, og_hops = spread("og", after(out_grad, normed2[0][1], normed2[0][n - 1]))

    cross_q, cross_mix, cross_total, state3 = [], [], [], []
    for c in range(CHUNKS):
        if c > 0:
            normed2[c] = after(normed2[c], sent, *og_hops[0])
        q = heads_of(product(normed2[c], full_cq).astype(BF).reshape(1, n * part, width))
        mix, total = attend(q, cross_k, cross_v, cross_allowed, scale)
        mix = mix.reshape(n, part, width)
        sent = whole(product(mix, full_cout).astype(BF))
        residual2 = state[c][0] + sink(f"r2_{c}", sent)[0]
        xhat3, rstd3 = norm_stats(residual2)
        cross_q.append(q)
        cross_mix.append(mix)
        cross_total.append(total)
        state3.append((residual2, xhat3, rstd3))
    normed3 = [
        spread(f"n3_{c}", (s[1] * norm_gains[2] + norm_shifts[2]).astype(BF))[0] for c, s in enumerate(state3)
    ]

    cat = lambda xs: jnp.concatenate(xs, axis=1)
    acts, grad_hiddens, parts3 = [], [], []
    for c, rows in enumerate(chunks):
        if c > 0:
            normed3[c] = after(normed3[c], parts3[c - 1])
        hidden = product(normed3[c], full_up)
        grad_rows = grad_all[:, rows]
        acted, gelu_back = jax.vjp(jax.nn.gelu, hidden)
        grad_hidden = gelu_back(right_inner(grad_rows, full_down))[0].astype(BF)
        if c > 0:
            grad_hidden = after(grad_hidden, *hops3[0])
        acts.append(acted.astype(BF))
        grad_hiddens.append(grad_hidden)
        parts3.append(whole(right_inner(grad_hidden, full_up).astype(BF)))
        if c == 0:
            grad_n3, hops3 = sink("d3_0", parts3[0])
            grad_n3s = [grad_n3]
    down_parts = [whole(product(after(acted, parts3[-1]), full_down).astype(BF)) for acted in acts]

    late = {}

    def down_weight(hop):
        every = cat([grad_all[:, rows] for rows in chunks])
        late["down"] = whole(left_inner(after(cat(acts), *hop, *down_parts), every).astype(BF))
        return (late["down"],)

    for c in range(1, CHUNKS):
        grad_n3, hops3 = sink(f"d3_{c}", parts3[c], {2: down_parts, 3: down_weight} if c == CHUNKS - 1 else {})
        grad_n3s.append(grad_n3)
    grad_down = late["down"]
    grad_up = whole(left_inner(after(cat(normed3), *hops3[1]), cat(grad_hiddens)).astype(BF))
    own_down = to_columns(grad_down)
    own_up = to_rows(grad_up)
    grad2, sums3, e2 = [], [], []
    for c, rows in enumerate(chunks):
        _, xhat3, rstd3 = state3[c]
        sums3.append(norm_sums(grad_n3s[c], xhat3))
        grad2.append(
            out_grad[rows].astype(F32) + norm_back(grad_n3s[c], xhat3, rstd3, norm_gains[2])
        )
        e2.append(spread(f"e2_{c}", grad2[c].astype(BF), {1: (grad_up,) if c > 0 else ()})[0])

    all_parts = [jnp.concatenate([p[k] for p in down_parts]) for k in range(n)]
    out_sum, out_hops = sink("out", all_parts, {1: (e2[-1][1], e2[-1][n - 1])})
    block_out = (jnp.concatenate([s[0] for s in state3]) + out_sum).astype(BF)
    parts2, grad_cqs, grad_ck, grad_cv = [], [], 0.0, 0.0
    for c in range(CHUNKS):
        if c > 0:
            e2[c] = after(e2[c], parts2[c - 1])
        grad_mix = right_inner(e2[c], full_cout).astype(BF).reshape(1, n * part, width)
        if c > 0:
            grad_mix = after(grad_mix, *out_hops[0])
        gq, gk, gv = attend_back(
            cross_q[c], cross_k, cross_v, cross_allowed, cross_total[c], heads_of(grad_mix), scale
        )
        gq = gq.reshape(n, part, width)
        grad_cqs.append(gq)
        grad_ck = grad_ck + gk
        grad_cv = grad_cv + gv
        parts2.append(whole(right_inner(gq, full_cq).astype(BF)))
    grad_ckv = jnp.concatenate(
        [grad_ck.reshape(text_count, width), grad_cv.reshape(text_count, width)], axis=1
    ).astype(BF)
    def cross_weights(hop):
        late["cout"] = whole(left_inner(after(cat(cross_mix), own_down, *hop), cat(e2)).astype(BF))
        late["cq"] = whole(left_inner(cat(normed2), after(cat(grad_cqs), *hop)).astype(BF))
        return late["cout"], late["cq"]

    grad1, sums2, e1 = [], [], []
    for c in range(CHUNKS):
        last = c == CHUNKS - 1
        grad_n2, hops2 = sink(f"d2_{c}", parts2[c], {2: (grad_ckv,), 3: cross_weights} if last else {})
        _, xhat2, rstd2 = state[c]
        sums2.append(norm_sums(grad_n2, xhat2))
        grad1.append(grad2[c] + norm_back(grad_n2, xhat2, rstd2, norm_gains[1]))
        if last:
            grad_wckv = whole(left_inner(text_rows, after(grad_ckv, own_up, *hops2[1])).astype(BF))
            grad_text_part = whole(
                right_inner(after(grad_ckv, *hops2[1]), full_ckv).astype(BF).reshape(n, -1, text.shape[2])
            )
        e1.append(spread(f"e1_{c}", grad1[c].astype(BF), {1: (grad_wckv,), 2: (grad_text_part,)} if last else {})[0])
    own_cout = to_columns(late["cout"])
    own_cq = to_rows(late["cq"])
    own_ckv = to_rows(grad_wckv)

    grad_text, text_hops = sink("text", grad_text_part, {1: (e1[-1][1], e1[-1][n - 1])})
    grad_text = grad_text.astype(BF)
    odd = [k for k in range(n) if k != 0 and k != n // 2]
    even = [0, n // 2]
    pieces = [None] * n
    grad_parts = [None] * n
    for group, which in enumerate((odd, even)):
        pick = lambda x: jnp.stack([x[k] for k in which])
        grad_mix = cat([right_inner(pick(e), full_out).astype(BF) for e in e1])
        if group > 0:
            grad_mix = after(grad_mix, back, own_cout, own_cq)
        gq, gk, gv = attend_back(
            pick(self_q), pick(self_k), pick(self_v), pick(self_allowed), pick(self_total), heads_of(grad_mix), scale
        )
        grads = jnp.concatenate(
            [g.astype(BF).reshape(len(which), PIX, width) for g in (gq, gk, gv)], axis=-1
        )
        moved = text_hops[0] if group == 0 else ()
        back = whole(right_inner(after(grads, *moved), full_qkv).astype(BF))
        for i, k in enumerate(which):
            pieces[k] = grads[i]
            grad_parts[k] = back[i]
    grad_n1, hops1 = sink("d1", grad_parts)
    grad_qkv = after(jnp.stack(pieces), *hops1[0])
    grad_wqkv = left_inner(normed1, grad_qkv)
    grad_out = sum(left_inner(self_mix[:, rows], e) for rows, e in zip(chunks, e1))
    grad1 = jnp.concatenate(grad1)
    grad_tokens = (grad1 + norm_back(grad_n1, xhat1, rstd1, norm_gains[0])).astype(BF)
    sums = lax.psum(
        jnp.stack([norm_sums(grad_n1, xhat1), sum(sums2), sum(sums3)]), ("wide", "narrow")
    )

    own_out = to_columns(grad_out)
    own_qkv = to_rows(grad_wqkv)
    return (
        block_out,
        grad_tokens,
        grad_text,
        sums[:, 0],
        sums[:, 1],
        own_qkv[:, :width],
        own_qkv[:, width : 2 * width],
        own_qkv[:, 2 * width :],
        own_out,
        own_cq,
        own_ckv[:, :width],
        own_ckv[:, width:],
        own_cout,
        own_up,
        own_down,
    )

def solution(mesh):
    in_specs = (
        P(("wide", "narrow"), None),
        P(("wide", "narrow"), None),
        P(("wide", "narrow"), None),
        P("wide", None),
        P("wide", None),
        P(),
        P(),
        P("wide", "narrow"),
        P("wide", "narrow"),
        P("wide", "narrow"),
        P("narrow", "wide"),
        P("wide", "narrow"),
        P("wide", "narrow"),
        P("wide", "narrow"),
        P("narrow", "wide"),
        P("wide", "narrow"),
        P("narrow", "wide"),
    )
    out_specs = (
        P(("wide", "narrow"), None),
        P(("wide", "narrow"), None),
        P(("wide", "narrow"), None),
        P(),
        P(),
        P("wide", "narrow"),
        P("wide", "narrow"),
        P("wide", "narrow"),
        P("narrow", "wide"),
        P("wide", "narrow"),
        P("wide", "narrow"),
        P("wide", "narrow"),
        P("narrow", "wide"),
        P("wide", "narrow"),
        P("narrow", "wide"),
    )
    return jax.shard_map(body, mesh=mesh, in_specs=in_specs, out_specs=out_specs, check_vma=False)
```

```python
import jax
import jax.numpy as jnp
from jax import lax
from jax.sharding import PartitionSpec as P

HEAD_DIM = 128
PIX = 256
CHUNKS = 2

EPSILON = 1e-06
MASKED = -1000000000.0
BF = jnp.bfloat16
F32 = jnp.float32


def product(left_side, right_side):
    return lax.dot_general(
        left_side,
        right_side,
        (((left_side.ndim - 1,), (0,)), ((), ())),
        preferred_element_type=F32,
    )


def right_inner(left_side, right_side):
    return lax.dot_general(
        left_side,
        right_side,
        (((left_side.ndim - 1,), (1,)), ((), ())),
        preferred_element_type=F32,
    )


def left_inner(left_side, right_side):
    rows = tuple(range(left_side.ndim - 1))
    return lax.dot_general(left_side, right_side, ((rows, rows), ((), ())), preferred_element_type=F32)


def spread(rows):
    n = lax.axis_size("narrow")
    here = lax.axis_index("narrow")
    up, down = [rows], [rows]
    for step in range(1, n):
        up.append(lax.ppermute(up[-1], "narrow", [(k, k + 1) for k in range(step - 1, n - 1)]))
        down.append(lax.ppermute(down[-1], "narrow", [(k, k - 1) for k in range(1, n - step + 1)]))
    parts = [rows] + [jnp.where(here >= s, up[s], down[n - s]) for s in range(1, n)]
    return jnp.stack(parts)


def sink(parts):
    n = lax.axis_size("narrow")
    up = down = None
    for step in range(1, n):
        one, other = parts[step], parts[n - step]
        if up is not None:
            one = up.astype(F32) + one.astype(F32)
            other = down.astype(F32) + other.astype(F32)
        up = lax.ppermute(one.astype(BF), "narrow", [(k, k + 1) for k in range(step)])
        down = lax.ppermute(other.astype(BF), "narrow", [(k, k - 1) for k in range(n - step, n)])
    return up.astype(F32) + down.astype(F32) + parts[0].astype(F32)


def norm_stats(features):
    center = features - jnp.mean(features, axis=-1, keepdims=True)
    rstd = lax.rsqrt(jnp.mean(center * center, axis=-1, keepdims=True) + EPSILON)
    return center * rstd, rstd


def norm_back(grad, xhat, rstd, gain):
    scaled = grad * gain
    return rstd * (
        scaled
        - jnp.mean(scaled, axis=-1, keepdims=True)
        - xhat * jnp.mean(scaled * xhat, axis=-1, keepdims=True)
    )


def norm_sums(grad, xhat):
    return jnp.stack([jnp.sum(grad * xhat, axis=0), jnp.sum(grad, axis=0)])


def score_block(queries, keys_in, allowed, score_scale):
    raw = jnp.einsum("iphe,iqhe->ihpq", queries, keys_in, preferred_element_type=F32)
    return jnp.where(allowed[:, None], raw * score_scale, MASKED)


def attend(queries, keys_in, values_in, allowed, score_scale):
    scores = score_block(queries, keys_in, allowed, score_scale)
    log_total = jax.nn.logsumexp(scores, axis=-1, keepdims=True)
    soft = jnp.exp(scores - log_total).astype(BF)
    mixture = jnp.einsum("ihpq,iqhe->iphe", soft, values_in, preferred_element_type=F32)
    return mixture.astype(BF), log_total


def attend_back(queries, keys_in, values_in, allowed, log_total, grad_mix, score_scale):
    soft = jnp.exp(score_block(queries, keys_in, allowed, score_scale) - log_total)
    grad_soft = jnp.einsum("iphe,iqhe->ihpq", grad_mix, values_in, preferred_element_type=F32)
    grad_values = jnp.einsum("ihpq,iphe->iqhe", soft.astype(BF), grad_mix, preferred_element_type=F32)
    row_dot = jnp.sum(soft * grad_soft, axis=-1, keepdims=True)
    grad_scores = (soft * (grad_soft - row_dot) * score_scale).astype(BF)
    grad_queries = jnp.einsum("ihpq,iqhe->iphe", grad_scores, keys_in, preferred_element_type=F32)
    grad_keys = jnp.einsum("ihpq,iphe->iqhe", grad_scores, queries, preferred_element_type=F32)
    return grad_queries.astype(BF), grad_keys, grad_values


def after(value, *others):
    return lax.optimization_barrier((value, *others))[0]


def follow(value, other):
    return value + (other[(0,) * other.ndim].astype(F32) * 0.0).astype(value.dtype)


def exchange_sum(value):
    for axis in ("wide", "narrow"):
        size = lax.axis_size(axis)
        step = 1
        while step < size:
            value = value + lax.ppermute(value, axis, [(k, k ^ step) for k in range(size)])
            step *= 2
    return value


def body(
    tokens,
    out_grad,
    captions,
    image_blocks,
    caption_owner,
    norm_gains,
    norm_shifts,
    w_query,
    w_key,
    w_value,
    w_out,
    w_cross_query,
    w_cross_key,
    w_cross_value,
    w_cross_out,
    w_up,
    w_down,
):
    scale = HEAD_DIM ** (-0.5)
    n = lax.axis_size("narrow")
    here = lax.axis_index("narrow")
    width = w_query.shape[1]
    heads = width // HEAD_DIM
    part = PIX // CHUNKS
    chunks = [slice(c * part, (c + 1) * part) for c in range(CHUNKS)]
    image_of = (here - jnp.arange(n)) % n

    def relative(blocks):
        return jnp.stack([lax.dynamic_index_in_dim(blocks, image_of[s], 0, False) for s in range(n)])

    def rows_of(*pieces):
        return lax.all_gather(
            jnp.concatenate([p.astype(BF) for p in pieces], axis=1), "wide", axis=0, tiled=True
        )

    def columns_of(piece):
        return lax.all_gather(piece.astype(BF), "wide", axis=1, tiled=True)

    def to_rows(g):
        return lax.psum_scatter(g.astype(BF), "wide", scatter_dimension=0, tiled=True).astype(F32)

    def to_columns(g):
        return lax.psum_scatter(g.astype(BF), "wide", scatter_dimension=1, tiled=True).astype(F32)

    full_qkv = rows_of(w_query, w_key, w_value)
    full_out = columns_of(w_out)
    full_ckv = rows_of(w_cross_key, w_cross_value)
    full_cq = rows_of(w_cross_query)
    full_cout = columns_of(w_cross_out)
    full_up = rows_of(w_up)
    full_down = columns_of(w_down)

    residual0 = tokens.astype(F32)
    xhat1, rstd1 = norm_stats(residual0)
    own1 = (xhat1 * norm_gains[0] + norm_shifts[0]).astype(BF)
    normed1 = spread(own1)
    qkv = product(normed1, full_qkv).astype(BF)
    heads_of = lambda x: x.reshape(x.shape[:-1] + (x.shape[-1] // HEAD_DIM, HEAD_DIM))
    self_q, self_k, self_v = [heads_of(qkv[..., k * width : (k + 1) * width]) for k in range(3)]
    blocks = image_blocks[image_of]
    self_allowed = blocks[:, :, None] == blocks[:, None, :]
    self_mix, self_total = attend(self_q, self_k, self_v, self_allowed, scale)
    self_mix = self_mix.reshape(n, PIX, width)

    text_rows = lax.all_gather(captions, "narrow", axis=0, tiled=True)
    text_count, text_width = text_rows.shape
    ckv = product(text_rows, full_ckv).astype(BF)
    cross_k = heads_of(ckv[None, :, :width])
    cross_v = heads_of(ckv[None, :, width:])
    owner = caption_owner[0]
    part_image = jnp.repeat(image_of, part)
    cross_allowed = (part_image[:, None] == owner[None, :])[None]

    state = []
    for rows in chunks:
        residual1 = residual0[rows] + sink(product(self_mix[:, rows], full_out).astype(BF))
        xhat2, rstd2 = norm_stats(residual1)
        state.append((residual1, xhat2, rstd2))
    normed2 = [spread((s[1] * norm_gains[1] + norm_shifts[1]).astype(BF)) for s in state]
    grad_all = relative(lax.all_gather(out_grad, "narrow", axis=0))

    cross_q, cross_mix, cross_total, state3 = [], [], [], []
    for c in range(CHUNKS):
        q = heads_of(product(normed2[c], full_cq).astype(BF).reshape(1, n * part, width))
        mix, total = attend(q, cross_k, cross_v, cross_allowed, scale)
        mix = mix.reshape(n, part, width)
        residual2 = state[c][0] + sink(product(mix, full_cout).astype(BF))
        xhat3, rstd3 = norm_stats(residual2)
        cross_q.append(q)
        cross_mix.append(mix)
        cross_total.append(total)
        state3.append((residual2, xhat3, rstd3))
    normed3 = [spread((s[1] * norm_gains[2] + norm_shifts[2]).astype(BF)) for s in state3]

    out_parts, acts, grad_hiddens, grad2, sums3 = [], [], [], [], []
    for c, rows in enumerate(chunks):
        if c > 0:
            normed3[c] = follow(normed3[c], sent)
        hidden = product(normed3[c], full_up)
        grad_rows = grad_all[:, rows]
        acted, gelu_back = jax.vjp(jax.nn.gelu, hidden)
        acted = acted.astype(BF)
        grad_hidden = gelu_back(right_inner(grad_rows, full_down))[0].astype(BF)
        acts.append(acted)
        grad_hiddens.append(grad_hidden)
        sent = lax.optimization_barrier(right_inner(grad_hidden, full_up).astype(BF))
        grad_n3 = sink(sent)
        residual2, xhat3, rstd3 = state3[c]
        sums3.append(norm_sums(grad_n3, xhat3))
        grad2.append(out_grad[rows].astype(F32) + norm_back(grad_n3, xhat3, rstd3, norm_gains[2]))
        out_parts.append(product(acted, full_down).astype(BF))
    cat = lambda xs: jnp.concatenate(xs, axis=1)
    acted, grad_hidden, n3 = cat(acts), cat(grad_hiddens), cat(normed3)
    grad_down = left_inner(acted, cat([grad_all[:, rows] for rows in chunks]))
    grad_up = left_inner(n3, grad_hidden)

    out_sum = lax.psum_scatter(relative(cat(out_parts)), "narrow", scatter_dimension=0)
    block_out = (jnp.concatenate([s[0] for s in state3]) + out_sum.astype(F32)).astype(BF)

    e2 = [spread(g.astype(BF)) for g in grad2]
    own_down = to_columns(grad_down)
    own_up = to_rows(grad_up)
    e2[-1] = after(e2[-1], grad_down, grad_up)
    grad1, sums2, grad_cqs, grad_ck, grad_cv = [], [], [], 0.0, 0.0
    for c in range(CHUNKS):
        grad_mix = heads_of(right_inner(e2[c], full_cout).astype(BF).reshape(1, n * part, width))
        gq, gk, gv = attend_back(
            cross_q[c], cross_k, cross_v, cross_allowed, cross_total[c], grad_mix, scale
        )
        gq = gq.reshape(n, part, width)
        grad_cqs.append(gq)
        grad_ck = grad_ck + gk
        grad_cv = grad_cv + gv
        grad_n2 = sink(right_inner(gq, full_cq).astype(BF))
        _, xhat2, rstd2 = state[c]
        sums2.append(norm_sums(grad_n2, xhat2))
        grad1.append(grad2[c] + norm_back(grad_n2, xhat2, rstd2, norm_gains[1]))
    grad_cout = left_inner(cat(cross_mix), cat(e2))
    grad_cq = left_inner(cat(normed2), cat(grad_cqs))
    grad_ckv = jnp.concatenate(
        [grad_ck.reshape(text_count, width), grad_cv.reshape(text_count, width)], axis=1
    ).astype(BF)
    grad_text_part = right_inner(grad_ckv, full_ckv).astype(BF).reshape(n, -1, text_width)
    grad_wckv = left_inner(text_rows, grad_ckv)

    e1 = [spread(g.astype(BF)) for g in grad1]
    own_cout = to_columns(grad_cout)
    own_cq = to_rows(grad_cq)
    own_ckv = to_rows(grad_wckv)
    e1[-1] = after(e1[-1], grad_cout, grad_cq, grad_wckv, grad_text_part)
    grad_mix = heads_of(cat([right_inner(e, full_out).astype(BF) for e in e1]))
    grad_mix = after(grad_mix, own_down, own_up)
    gq, gk, gv = attend_back(self_q, self_k, self_v, self_allowed, self_total, grad_mix, scale)
    grad_qkv = jnp.concatenate(
        [g.astype(BF).reshape(n, PIX, width) for g in (gq, gk, gv)], axis=-1
    )
    grad_out = left_inner(self_mix, cat(e1))
    grad_wqkv = left_inner(normed1, grad_qkv)
    grad_n1 = sink(right_inner(after(grad_qkv, grad_wqkv), full_qkv).astype(BF))
    grad_text = sink(relative(after(grad_text_part, grad_mix))).astype(BF)
    grad1 = jnp.concatenate(grad1)
    grad_n1 = after(grad_n1, own_cout, own_cq, own_ckv)
    grad_tokens = (grad1 + norm_back(grad_n1, xhat1, rstd1, norm_gains[0])).astype(BF)
    sums = exchange_sum(jnp.stack([norm_sums(grad_n1, xhat1), sum(sums2), sum(sums3)]))

    own_out = to_columns(grad_out)
    own_qkv = to_rows(grad_wqkv)
    return (
        block_out,
        grad_tokens,
        grad_text,
        sums[:, 0],
        sums[:, 1],
        own_qkv[:, :width],
        own_qkv[:, width : 2 * width],
        own_qkv[:, 2 * width :],
        own_out,
        own_cq,
        own_ckv[:, :width],
        own_ckv[:, width:],
        own_cout,
        own_up,
        own_down,
    )

def solution(mesh):
    in_specs = (
        P(("wide", "narrow"), None),
        P(("wide", "narrow"), None),
        P(("wide", "narrow"), None),
        P("wide", None),
        P("wide", None),
        P(),
        P(),
        P("wide", "narrow"),
        P("wide", "narrow"),
        P("wide", "narrow"),
        P("narrow", "wide"),
        P("wide", "narrow"),
        P("wide", "narrow"),
        P("wide", "narrow"),
        P("narrow", "wide"),
        P("wide", "narrow"),
        P("narrow", "wide"),
    )
    out_specs = (
        P(("wide", "narrow"), None),
        P(("wide", "narrow"), None),
        P(("wide", "narrow"), None),
        P(),
        P(),
        P("wide", "narrow"),
        P("wide", "narrow"),
        P("wide", "narrow"),
        P("narrow", "wide"),
        P("wide", "narrow"),
        P("wide", "narrow"),
        P("wide", "narrow"),
        P("narrow", "wide"),
        P("wide", "narrow"),
        P("narrow", "wide"),
    )
    return jax.shard_map(body, mesh=mesh, in_specs=in_specs, out_specs=out_specs, check_vma=False)
```

```python
import jax
import jax.numpy as jnp
from jax import lax
from jax.sharding import PartitionSpec as P

HEAD_DIM = 128
PIX = 256
CHUNKS = 2

EPSILON = 1e-06
MASKED = -1000000000.0
BF = jnp.bfloat16
F32 = jnp.float32


def product(left_side, right_side):
    return lax.dot_general(
        left_side,
        right_side,
        (((left_side.ndim - 1,), (0,)), ((), ())),
        preferred_element_type=F32,
    )


def right_inner(left_side, right_side):
    return lax.dot_general(
        left_side,
        right_side,
        (((left_side.ndim - 1,), (1,)), ((), ())),
        preferred_element_type=F32,
    )


def left_inner(left_side, right_side):
    rows = tuple(range(left_side.ndim - 1))
    return lax.dot_general(left_side, right_side, ((rows, rows), ((), ())), preferred_element_type=F32)


def follow(value, *others):
    if not others:
        return value
    nothing = sum(o[(0,) * o.ndim].astype(F32) for o in others) * 0.0
    return value + nothing.astype(value.dtype)


def whole(value):
    return lax.optimization_barrier(value)


def after(value, *others):
    return lax.optimization_barrier((value, *others))[0]


def spread(name, rows, gates={}):
    n = lax.axis_size("narrow")
    here = lax.axis_index("narrow")
    with jax.named_scope("spread_" + name):
        up, down = [rows], [rows]
        for step in range(1, n):
            one, other = follow(up[-1], *gates.get(step, ())), follow(down[-1], *gates.get(step, ()))
            up.append(lax.ppermute(one, "narrow", [(k, k + 1) for k in range(step - 1, n - 1)]))
            down.append(lax.ppermute(other, "narrow", [(k, k - 1) for k in range(1, n - step + 1)]))
        parts = [rows] + [jnp.where(here >= s, up[s], down[n - s]) for s in range(1, n)]
        return jnp.stack(parts), [(up[s], down[s]) for s in range(1, n)]


def sink(name, parts, gates={}):
    n = lax.axis_size("narrow")
    hops = []
    with jax.named_scope("sink_" + name):
        for step in range(1, n):
            one, other = parts[step], parts[n - step]
            gate = gates.get(step, ())
            if callable(gate):
                gate = gate(hops[0])
            if hops:
                one = hops[-1][0].astype(F32) + one.astype(F32)
                other = hops[-1][1].astype(F32) + other.astype(F32)
            one, other = follow(one, *gate), follow(other, *gate)
            up = lax.ppermute(one.astype(BF), "narrow", [(k, k + 1) for k in range(step)])
            down = lax.ppermute(other.astype(BF), "narrow", [(k, k - 1) for k in range(n - step, n)])
            hops.append((up, down))
        return up.astype(F32) + down.astype(F32) + parts[0].astype(F32), hops


def norm_stats(features):
    center = features - jnp.mean(features, axis=-1, keepdims=True)
    rstd = lax.rsqrt(jnp.mean(center * center, axis=-1, keepdims=True) + EPSILON)
    return center * rstd, rstd


def norm_back(grad, xhat, rstd, gain):
    scaled = grad * gain
    return rstd * (
        scaled
        - jnp.mean(scaled, axis=-1, keepdims=True)
        - xhat * jnp.mean(scaled * xhat, axis=-1, keepdims=True)
    )


def norm_sums(grad, xhat):
    return jnp.stack([jnp.sum(grad * xhat, axis=0), jnp.sum(grad, axis=0)])


def score_block(queries, keys_in, allowed, score_scale):
    raw = jnp.einsum("iphe,iqhe->ihpq", queries, keys_in, preferred_element_type=F32)
    return jnp.where(allowed[:, None], raw * score_scale, MASKED)


def attend(queries, keys_in, values_in, allowed, score_scale):
    scores = score_block(queries, keys_in, allowed, score_scale)
    log_total = jax.nn.logsumexp(scores, axis=-1, keepdims=True)
    soft = jnp.exp(scores - log_total).astype(BF)
    mixture = jnp.einsum("ihpq,iqhe->iphe", soft, values_in, preferred_element_type=F32)
    return mixture.astype(BF), log_total


def attend_back(queries, keys_in, values_in, allowed, log_total, grad_mix, score_scale):
    soft = jnp.exp(score_block(queries, keys_in, allowed, score_scale) - log_total)
    grad_soft = jnp.einsum("iphe,iqhe->ihpq", grad_mix, values_in, preferred_element_type=F32)
    grad_values = jnp.einsum("ihpq,iphe->iqhe", soft.astype(BF), grad_mix, preferred_element_type=F32)
    row_dot = jnp.sum(soft * grad_soft, axis=-1, keepdims=True)
    grad_scores = (soft * (grad_soft - row_dot) * score_scale).astype(BF)
    grad_queries = jnp.einsum("ihpq,iqhe->iphe", grad_scores, keys_in, preferred_element_type=F32)
    grad_keys = jnp.einsum("ihpq,iphe->iqhe", grad_scores, queries, preferred_element_type=F32)
    return grad_queries.astype(BF), grad_keys, grad_values


def body(
    tokens,
    out_grad,
    captions,
    image_blocks,
    caption_owner,
    norm_gains,
    norm_shifts,
    w_query,
    w_key,
    w_value,
    w_out,
    w_cross_query,
    w_cross_key,
    w_cross_value,
    w_cross_out,
    w_up,
    w_down,
):
    scale = HEAD_DIM ** (-0.5)
    n = lax.axis_size("narrow")
    here = lax.axis_index("narrow")
    width = w_query.shape[1]
    heads = width // HEAD_DIM
    part = PIX // CHUNKS
    chunks = [slice(c * part, (c + 1) * part) for c in range(CHUNKS)]
    image_of = (here - jnp.arange(n)) % n

    def rows_of(*pieces):
        return lax.all_gather(
            jnp.concatenate([p.astype(BF) for p in pieces], axis=1), "wide", axis=0, tiled=True
        )

    def columns_of(piece):
        return lax.all_gather(piece.astype(BF), "wide", axis=1, tiled=True)

    def to_rows(g):
        return lax.psum_scatter(g.astype(BF), "wide", scatter_dimension=0, tiled=True).astype(F32)

    def to_columns(g):
        return lax.psum_scatter(g.astype(BF), "wide", scatter_dimension=1, tiled=True).astype(F32)

    full_qkv = rows_of(w_query, w_key, w_value)
    full_out = columns_of(w_out)
    full_ckv = rows_of(w_cross_key, w_cross_value)
    full_cq = rows_of(w_cross_query)
    full_cout = columns_of(w_cross_out)
    full_up = rows_of(w_up)
    full_down = columns_of(w_down)

    residual0 = tokens.astype(F32)
    xhat1, rstd1 = norm_stats(residual0)
    own1 = (xhat1 * norm_gains[0] + norm_shifts[0]).astype(BF)
    normed1 = spread("n1", own1)[0]
    qkv = product(normed1, full_qkv).astype(BF)
    heads_of = lambda x: x.reshape(x.shape[:-1] + (x.shape[-1] // HEAD_DIM, HEAD_DIM))
    self_q, self_k, self_v = [heads_of(qkv[..., k * width : (k + 1) * width]) for k in range(3)]
    blocks = image_blocks[image_of]
    self_allowed = blocks[:, :, None] == blocks[:, None, :]
    self_mix, self_total = attend(self_q, self_k, self_v, self_allowed, scale)
    self_mix = self_mix.reshape(n, PIX, width)

    text = spread("text", follow(captions, normed1[1], normed1[n - 1]), {2: (self_mix,)})[0]
    text_count = text.shape[0] * text.shape[1]
    text_rows = text.reshape(text_count, text.shape[2])
    ckv = product(text_rows, full_ckv).astype(BF)
    cross_k = heads_of(ckv[None, :, :width])
    cross_v = heads_of(ckv[None, :, width:])
    owner = caption_owner[0].reshape(n, -1)[image_of].reshape(-1)
    part_image = jnp.repeat(image_of, part)
    cross_allowed = (part_image[:, None] == owner[None, :])[None]

    state = []
    for c, rows in enumerate(chunks):
        residual1 = residual0[rows] + sink(f"r1_{c}", product(self_mix[:, rows], full_out).astype(BF))[0]
        xhat2, rstd2 = norm_stats(residual1)
        state.append((residual1, xhat2, rstd2))
    normed2 = [
        spread(f"n2_{c}", (s[1] * norm_gains[1] + norm_shifts[1]).astype(BF))[0] for c, s in enumerate(state)
    ]
    grad_all, og_hops = spread("og", follow(out_grad, normed2[0][1], normed2[0][n - 1]))

    cross_q, cross_mix, cross_total, state3 = [], [], [], []
    for c in range(CHUNKS):
        if c > 0:
            normed2[c] = follow(normed2[c], sent, *og_hops[0])
        q = heads_of(product(normed2[c], full_cq).astype(BF).reshape(1, n * part, width))
        mix, total = attend(q, cross_k, cross_v, cross_allowed, scale)
        mix = mix.reshape(n, part, width)
        sent = whole(product(mix, full_cout).astype(BF))
        residual2 = state[c][0] + sink(f"r2_{c}", sent, {1: og_hops[1]} if c > 0 else {})[0]
        xhat3, rstd3 = norm_stats(residual2)
        cross_q.append(q)
        cross_mix.append(mix)
        cross_total.append(total)
        state3.append((residual2, xhat3, rstd3))
    normed3 = [
        spread(f"n3_{c}", (s[1] * norm_gains[2] + norm_shifts[2]).astype(BF))[0] for c, s in enumerate(state3)
    ]

    out_parts, acts, grad_hiddens, grad2, sums3 = [], [], [], [], []
    for c, rows in enumerate(chunks):
        hidden = product(normed3[c], full_up)
        grad_rows = grad_all[:, rows]
        acted, gelu_back = jax.vjp(jax.nn.gelu, hidden)
        acted = acted.astype(BF)
        grad_hidden = gelu_back(right_inner(grad_rows, full_down))[0].astype(BF)
        acts.append(acted)
        grad_hiddens.append(grad_hidden)
        grad_n3 = sink(f"d3_{c}", right_inner(grad_hidden, full_up).astype(BF))[0]
        residual2, xhat3, rstd3 = state3[c]
        sums3.append(norm_sums(grad_n3, xhat3))
        grad2.append(out_grad[rows].astype(F32) + norm_back(grad_n3, xhat3, rstd3, norm_gains[2]))
        out_parts.append(whole(product(acted, full_down).astype(BF)))
    cat = lambda xs: jnp.concatenate(xs, axis=1)
    acted, grad_hidden, n3 = cat(acts), cat(grad_hiddens), cat(normed3)
    grad_down = left_inner(acted, cat([grad_all[:, rows] for rows in chunks]))
    grad_up = left_inner(n3, grad_hidden)

    e2, e2_hops = map(list, zip(*[spread(f"e2_{c}", g.astype(BF)) for c, g in enumerate(grad2)]))
    out_sum, out_hops = sink(
        "out", [jnp.concatenate([p[k] for p in out_parts]) for k in range(n)], {1: e2_hops[-1][1]}
    )
    block_out = (jnp.concatenate([s[0] for s in state3]) + out_sum).astype(BF)
    own_down = to_columns(grad_down)
    own_up = to_rows(grad_up)
    e2[-1] = after(e2[-1], grad_down, grad_up)
    grad1, sums2, grad_cqs, grad_ck, grad_cv = [], [], [], 0.0, 0.0
    for c in range(CHUNKS):
        grad_mix = heads_of(right_inner(e2[c], full_cout).astype(BF).reshape(1, n * part, width))
        gq, gk, gv = attend_back(
            cross_q[c], cross_k, cross_v, cross_allowed, cross_total[c], grad_mix, scale
        )
        gq = gq.reshape(n, part, width)
        grad_cqs.append(gq)
        grad_ck = grad_ck + gk
        grad_cv = grad_cv + gv
        sent = whole(right_inner(gq if c == 0 else follow(gq, *out_hops[0]), full_cq).astype(BF))
        grad_n2 = sink(f"d2_{c}", sent, {1: out_hops[1]} if c > 0 else {})[0]
        _, xhat2, rstd2 = state[c]
        sums2.append(norm_sums(grad_n2, xhat2))
        grad1.append(grad2[c] + norm_back(grad_n2, xhat2, rstd2, norm_gains[1]))
    grad_cout = left_inner(cat(cross_mix), cat(e2))
    grad_cq = left_inner(cat(normed2), cat(grad_cqs))
    grad_ckv = jnp.concatenate(
        [grad_ck.reshape(text_count, width), grad_cv.reshape(text_count, width)], axis=1
    ).astype(BF)
    grad_text_part = whole(right_inner(grad_ckv, full_ckv).astype(BF).reshape(n, -1, text.shape[2]))
    grad_wckv = left_inner(text_rows, grad_ckv)

    grad1[0] = follow(grad1[0], *out_hops[2])
    e1, e1_hops = map(list, zip(*[spread(f"e1_{c}", g.astype(BF)) for c, g in enumerate(grad1)]))
    own_cout = to_columns(grad_cout)
    own_cq = to_rows(grad_cq)
    own_ckv = to_rows(grad_wckv)
    e1[-1] = after(e1[-1], grad_cout, grad_cq, grad_wckv)
    grad_mix = heads_of(cat([right_inner(e, full_out).astype(BF) for e in e1]))
    grad_mix = after(grad_mix, own_down, own_up)
    gq, gk, gv = attend_back(self_q, self_k, self_v, self_allowed, self_total, grad_mix, scale)
    grad_text, text_hops = sink("text", grad_text_part, {1: e1_hops[-1][1], 2: (gq,)})
    grad_text = grad_text.astype(BF)
    grad_qkv = jnp.concatenate(
        [g.astype(BF).reshape(n, PIX, width) for g in (gq, gk, gv)], axis=-1
    )
    grad_qkv = follow(grad_qkv, *text_hops[0])
    grad_out = left_inner(self_mix, cat(e1))
    grad_wqkv = left_inner(normed1, grad_qkv)
    grad_n1_part = whole(right_inner(after(grad_qkv, grad_wqkv), full_qkv).astype(BF))
    grad_n1 = sink("d1", grad_n1_part, {1: text_hops[1]})[0]
    grad1 = jnp.concatenate(grad1)
    grad_n1 = after(grad_n1, own_cout, own_cq, own_ckv)
    grad_tokens = (grad1 + norm_back(grad_n1, xhat1, rstd1, norm_gains[0])).astype(BF)
    sums = lax.psum(
        jnp.stack([norm_sums(grad_n1, xhat1), sum(sums2), sum(sums3)]), ("wide", "narrow")
    )

    own_out = to_columns(grad_out)
    own_qkv = to_rows(grad_wqkv)
    return (
        block_out,
        grad_tokens,
        grad_text,
        sums[:, 0],
        sums[:, 1],
        own_qkv[:, :width],
        own_qkv[:, width : 2 * width],
        own_qkv[:, 2 * width :],
        own_out,
        own_cq,
        own_ckv[:, :width],
        own_ckv[:, width:],
        own_cout,
        own_up,
        own_down,
    )

def solution(mesh):
    in_specs = (
        P(("wide", "narrow"), None),
        P(("wide", "narrow"), None),
        P(("wide", "narrow"), None),
        P("wide", None),
        P("wide", None),
        P(),
        P(),
        P("wide", "narrow"),
        P("wide", "narrow"),
        P("wide", "narrow"),
        P("narrow", "wide"),
        P("wide", "narrow"),
        P("wide", "narrow"),
        P("wide", "narrow"),
        P("narrow", "wide"),
        P("wide", "narrow"),
        P("narrow", "wide"),
    )
    out_specs = (
        P(("wide", "narrow"), None),
        P(("wide", "narrow"), None),
        P(("wide", "narrow"), None),
        P(),
        P(),
        P("wide", "narrow"),
        P("wide", "narrow"),
        P("wide", "narrow"),
        P("narrow", "wide"),
        P("wide", "narrow"),
        P("wide", "narrow"),
        P("wide", "narrow"),
        P("narrow", "wide"),
        P("wide", "narrow"),
        P("narrow", "wide"),
    )
    return jax.shard_map(body, mesh=mesh, in_specs=in_specs, out_specs=out_specs, check_vma=False)
```

```python
import jax
import jax.numpy as jnp
from jax import lax
from jax.sharding import PartitionSpec as P

HEAD_DIM = 128
PIX = 256
CHUNKS = 2

EPSILON = 1e-06
MASKED = -1000000000.0
BF = jnp.bfloat16
F32 = jnp.float32


def product(left_side, right_side):
    return lax.dot_general(
        left_side,
        right_side,
        (((left_side.ndim - 1,), (0,)), ((), ())),
        preferred_element_type=F32,
    )


def right_inner(left_side, right_side):
    return lax.dot_general(
        left_side,
        right_side,
        (((left_side.ndim - 1,), (1,)), ((), ())),
        preferred_element_type=F32,
    )


def left_inner(left_side, right_side):
    rows = tuple(range(left_side.ndim - 1))
    return lax.dot_general(left_side, right_side, ((rows, rows), ((), ())), preferred_element_type=F32)


def follow(value, *others):
    if not others:
        return value
    nothing = sum(o[(0,) * o.ndim].astype(F32) for o in others) * 0.0
    return value + nothing.astype(value.dtype)


def whole(value):
    return lax.optimization_barrier(value)


def after(value, *others):
    return lax.optimization_barrier((value, *others))[0]


def spread(name, rows, gates={}):
    n = lax.axis_size("narrow")
    here = lax.axis_index("narrow")
    with jax.named_scope("spread_" + name):
        up, down = [rows], [rows]
        for step in range(1, n):
            one, other = follow(up[-1], *gates.get(step, ())), follow(down[-1], *gates.get(step, ()))
            up.append(lax.ppermute(one, "narrow", [(k, k + 1) for k in range(step - 1, n - 1)]))
            down.append(lax.ppermute(other, "narrow", [(k, k - 1) for k in range(1, n - step + 1)]))
        parts = [rows] + [jnp.where(here >= s, up[s], down[n - s]) for s in range(1, n)]
        return jnp.stack(parts), [(up[s], down[s]) for s in range(1, n)]


def sink(name, parts, gates={}, hops=(), until=None):
    n = lax.axis_size("narrow")
    hops = list(hops)
    with jax.named_scope("sink_" + name):
        for step in range(len(hops) + 1, until or n):
            one, other = parts[step], parts[n - step]
            if hops:
                one = hops[-1][0].astype(F32) + one.astype(F32)
                other = hops[-1][1].astype(F32) + other.astype(F32)
            one, other = follow(one, *gates.get(step, ())), follow(other, *gates.get(step, ()))
            up = lax.ppermute(one.astype(BF), "narrow", [(k, k + 1) for k in range(step)])
            down = lax.ppermute(other.astype(BF), "narrow", [(k, k - 1) for k in range(n - step, n)])
            hops.append((up, down))
        if until:
            return None, hops
        return up.astype(F32) + down.astype(F32) + parts[0].astype(F32), hops


def norm_stats(features):
    center = features - jnp.mean(features, axis=-1, keepdims=True)
    rstd = lax.rsqrt(jnp.mean(center * center, axis=-1, keepdims=True) + EPSILON)
    return center * rstd, rstd


def norm_back(grad, xhat, rstd, gain):
    scaled = grad * gain
    return rstd * (
        scaled
        - jnp.mean(scaled, axis=-1, keepdims=True)
        - xhat * jnp.mean(scaled * xhat, axis=-1, keepdims=True)
    )


def norm_sums(grad, xhat):
    return jnp.stack([jnp.sum(grad * xhat, axis=0), jnp.sum(grad, axis=0)])


def score_block(queries, keys_in, allowed, score_scale):
    raw = jnp.einsum("iphe,iqhe->ihpq", queries, keys_in, preferred_element_type=F32)
    return jnp.where(allowed[:, None], raw * score_scale, MASKED)


def attend(queries, keys_in, values_in, allowed, score_scale):
    scores = score_block(queries, keys_in, allowed, score_scale)
    log_total = jax.nn.logsumexp(scores, axis=-1, keepdims=True)
    soft = jnp.exp(scores - log_total).astype(BF)
    mixture = jnp.einsum("ihpq,iqhe->iphe", soft, values_in, preferred_element_type=F32)
    return mixture.astype(BF), log_total


def attend_back(queries, keys_in, values_in, allowed, log_total, grad_mix, score_scale):
    soft = jnp.exp(score_block(queries, keys_in, allowed, score_scale) - log_total)
    grad_soft = jnp.einsum("iphe,iqhe->ihpq", grad_mix, values_in, preferred_element_type=F32)
    grad_values = jnp.einsum("ihpq,iphe->iqhe", soft.astype(BF), grad_mix, preferred_element_type=F32)
    row_dot = jnp.sum(soft * grad_soft, axis=-1, keepdims=True)
    grad_scores = (soft * (grad_soft - row_dot) * score_scale).astype(BF)
    grad_queries = jnp.einsum("ihpq,iqhe->iphe", grad_scores, keys_in, preferred_element_type=F32)
    grad_keys = jnp.einsum("ihpq,iphe->iqhe", grad_scores, queries, preferred_element_type=F32)
    return grad_queries.astype(BF), grad_keys, grad_values


def body(
    tokens,
    out_grad,
    captions,
    image_blocks,
    caption_owner,
    norm_gains,
    norm_shifts,
    w_query,
    w_key,
    w_value,
    w_out,
    w_cross_query,
    w_cross_key,
    w_cross_value,
    w_cross_out,
    w_up,
    w_down,
):
    scale = HEAD_DIM ** (-0.5)
    n = lax.axis_size("narrow")
    here = lax.axis_index("narrow")
    width = w_query.shape[1]
    heads = width // HEAD_DIM
    part = PIX // CHUNKS
    chunks = [slice(c * part, (c + 1) * part) for c in range(CHUNKS)]
    image_of = (here - jnp.arange(n)) % n

    def rows_of(*pieces):
        return lax.all_gather(
            jnp.concatenate([p.astype(BF) for p in pieces], axis=1), "wide", axis=0, tiled=True
        )

    def columns_of(piece):
        return lax.all_gather(piece.astype(BF), "wide", axis=1, tiled=True)

    def to_rows(g):
        return lax.psum_scatter(g.astype(BF), "wide", scatter_dimension=0, tiled=True).astype(F32)

    def to_columns(g):
        return lax.psum_scatter(g.astype(BF), "wide", scatter_dimension=1, tiled=True).astype(F32)

    full_qkv = rows_of(w_query, w_key, w_value)

    residual0 = tokens.astype(F32)
    xhat1, rstd1 = norm_stats(residual0)
    own1 = (xhat1 * norm_gains[0] + norm_shifts[0]).astype(BF)
    full_out = columns_of(w_out)
    full_ckv = rows_of(w_cross_key, w_cross_value)
    full_cq = rows_of(w_cross_query)
    full_cout = columns_of(w_cross_out)
    full_up = rows_of(w_up)
    full_down = columns_of(w_down)
    normed1 = spread("n1", own1)[0]
    qkv = product(normed1, full_qkv).astype(BF)
    heads_of = lambda x: x.reshape(x.shape[:-1] + (x.shape[-1] // HEAD_DIM, HEAD_DIM))
    self_q, self_k, self_v = [heads_of(qkv[..., k * width : (k + 1) * width]) for k in range(3)]
    blocks = image_blocks[image_of]
    self_allowed = blocks[:, :, None] == blocks[:, None, :]
    self_mix, self_total = attend(self_q, self_k, self_v, self_allowed, scale)
    self_mix = self_mix.reshape(n, PIX, width)

    text = spread("text", follow(captions, normed1[1], normed1[n - 1]), {2: (self_mix,)})[0]
    text_count = text.shape[0] * text.shape[1]
    text_rows = text.reshape(text_count, text.shape[2])
    ckv = product(text_rows, full_ckv).astype(BF)
    cross_k = heads_of(ckv[None, :, :width])
    cross_v = heads_of(ckv[None, :, width:])
    owner = caption_owner[0].reshape(n, -1)[image_of].reshape(-1)
    part_image = jnp.repeat(image_of, part)
    cross_allowed = (part_image[:, None] == owner[None, :])[None]

    state = []
    for c, rows in enumerate(chunks):
        residual1 = residual0[rows] + sink(f"r1_{c}", product(self_mix[:, rows], full_out).astype(BF))[0]
        xhat2, rstd2 = norm_stats(residual1)
        state.append((residual1, xhat2, rstd2))
    normed2 = [
        spread(f"n2_{c}", (s[1] * norm_gains[1] + norm_shifts[1]).astype(BF))[0] for c, s in enumerate(state)
    ]
    grad_all, og_hops = spread("og", follow(out_grad, normed2[0][1], normed2[0][n - 1]))

    cross_q, cross_mix, cross_total, state3 = [], [], [], []
    for c in range(CHUNKS):
        if c > 0:
            normed2[c] = follow(normed2[c], sent, *og_hops[0])
        q = heads_of(product(normed2[c], full_cq).astype(BF).reshape(1, n * part, width))
        mix, total = attend(q, cross_k, cross_v, cross_allowed, scale)
        mix = mix.reshape(n, part, width)
        sent = whole(product(mix, full_cout).astype(BF))
        residual2 = state[c][0] + sink(f"r2_{c}", sent, {1: og_hops[1]} if c > 0 else {})[0]
        xhat3, rstd3 = norm_stats(residual2)
        cross_q.append(q)
        cross_mix.append(mix)
        cross_total.append(total)
        state3.append((residual2, xhat3, rstd3))
    normed3 = [
        spread(f"n3_{c}", (s[1] * norm_gains[2] + norm_shifts[2]).astype(BF))[0] for c, s in enumerate(state3)
    ]

    out_parts, acts, grad_hiddens, grad2, sums3 = [], [], [], [], []
    for c, rows in enumerate(chunks):
        hidden = product(normed3[c], full_up)
        grad_rows = grad_all[:, rows]
        acted, gelu_back = jax.vjp(jax.nn.gelu, hidden)
        acted = acted.astype(BF)
        grad_hidden = gelu_back(right_inner(grad_rows, full_down))[0].astype(BF)
        acts.append(acted)
        grad_hiddens.append(grad_hidden)
        grad_n3 = sink(f"d3_{c}", right_inner(grad_hidden, full_up).astype(BF))[0]
        residual2, xhat3, rstd3 = state3[c]
        sums3.append(norm_sums(grad_n3, xhat3))
        grad2.append(out_grad[rows].astype(F32) + norm_back(grad_n3, xhat3, rstd3, norm_gains[2]))
        out_parts.append(whole(product(acted, full_down).astype(BF)))
    cat = lambda xs: jnp.concatenate(xs, axis=1)
    acted, grad_hidden, n3 = cat(acts), cat(grad_hiddens), cat(normed3)
    grad_down = left_inner(acted, cat([grad_all[:, rows] for rows in chunks]))
    grad_up = left_inner(n3, grad_hidden)

    e2, e2_hops = map(list, zip(*[spread(f"e2_{c}", g.astype(BF)) for c, g in enumerate(grad2)]))
    out_parts = [jnp.concatenate([p[k] for p in out_parts]) for k in range(n)]
    out_hops = sink("out", out_parts, {1: e2_hops[-1][1]}, until=n - 1)[1]
    own_down = to_columns(grad_down)
    own_up = to_rows(grad_up)
    e2[-1] = after(e2[-1], grad_down, grad_up)
    grad1, sums2, grad_cqs, grad_ck, grad_cv = [], [], [], 0.0, 0.0
    for c in range(CHUNKS):
        grad_mix = heads_of(right_inner(e2[c], full_cout).astype(BF).reshape(1, n * part, width))
        gq, gk, gv = attend_back(
            cross_q[c], cross_k, cross_v, cross_allowed, cross_total[c], grad_mix, scale
        )
        gq = gq.reshape(n, part, width)
        grad_cqs.append(gq)
        grad_ck = grad_ck + gk
        grad_cv = grad_cv + gv
        sent = whole(right_inner(gq if c == 0 else follow(gq, *out_hops[0]), full_cq).astype(BF))
        grad_n2 = sink(f"d2_{c}", sent, {1: out_hops[1]} if c > 0 else {})[0]
        _, xhat2, rstd2 = state[c]
        sums2.append(norm_sums(grad_n2, xhat2))
        grad1.append(grad2[c] + norm_back(grad_n2, xhat2, rstd2, norm_gains[1]))
    grad_cout = left_inner(cat(cross_mix), cat(e2))
    grad_cq = left_inner(cat(normed2), cat(grad_cqs))
    grad_ckv = jnp.concatenate(
        [grad_ck.reshape(text_count, width), grad_cv.reshape(text_count, width)], axis=1
    ).astype(BF)
    grad_text_part = whole(right_inner(grad_ckv, full_ckv).astype(BF).reshape(n, -1, text.shape[2]))
    grad_wckv = left_inner(text_rows, grad_ckv)

    e1, e1_hops = map(list, zip(*[spread(f"e1_{c}", g.astype(BF)) for c, g in enumerate(grad1)]))
    own_cout = to_columns(grad_cout)
    own_cq = to_rows(grad_cq)
    own_ckv = to_rows(grad_wckv)
    e1[-1] = after(e1[-1], grad_cout, grad_cq, grad_wckv)
    grad_mix = heads_of(cat([right_inner(e, full_out).astype(BF) for e in e1]))
    grad_mix = after(grad_mix, own_down, own_up)
    gq, gk, gv = attend_back(self_q, self_k, self_v, self_allowed, self_total, grad_mix, scale)
    out_sum, out_hops = sink("out", out_parts, {n - 1: e1_hops[-1][1]}, out_hops)
    block_out = (jnp.concatenate([s[0] for s in state3]) + out_sum).astype(BF)
    grad_text, text_hops = sink("text", grad_text_part, {1: e1_hops[-1][1], 2: (gq,)})
    grad_text = grad_text.astype(BF)
    grad_qkv = jnp.concatenate(
        [g.astype(BF).reshape(n, PIX, width) for g in (gq, gk, gv)], axis=-1
    )
    grad_qkv = follow(grad_qkv, *text_hops[1])
    grad_out = left_inner(self_mix, cat(e1))
    grad_n1_part = whole(right_inner(grad_qkv, full_qkv).astype(BF))
    grad_n1 = sink("d1", grad_n1_part, {1: out_hops[-1]})[0]
    grad_wqkv = left_inner(normed1, after(grad_qkv, grad_n1_part))
    grad1 = jnp.concatenate(grad1)
    grad_n1 = after(grad_n1, own_cout, own_cq, own_ckv)
    grad_tokens = (grad1 + norm_back(grad_n1, xhat1, rstd1, norm_gains[0])).astype(BF)
    sums = lax.psum(
        jnp.stack([norm_sums(grad_n1, xhat1), sum(sums2), sum(sums3)]), ("wide", "narrow")
    )

    own_out = to_columns(grad_out)
    own_qkv = to_rows(grad_wqkv)
    return (
        block_out,
        grad_tokens,
        grad_text,
        sums[:, 0],
        sums[:, 1],
        own_qkv[:, :width],
        own_qkv[:, width : 2 * width],
        own_qkv[:, 2 * width :],
        own_out,
        own_cq,
        own_ckv[:, :width],
        own_ckv[:, width:],
        own_cout,
        own_up,
        own_down,
    )

def solution(mesh):
    in_specs = (
        P(("wide", "narrow"), None),
        P(("wide", "narrow"), None),
        P(("wide", "narrow"), None),
        P("wide", None),
        P("wide", None),
        P(),
        P(),
        P("wide", "narrow"),
        P("wide", "narrow"),
        P("wide", "narrow"),
        P("narrow", "wide"),
        P("wide", "narrow"),
        P("wide", "narrow"),
        P("wide", "narrow"),
        P("narrow", "wide"),
        P("wide", "narrow"),
        P("narrow", "wide"),
    )
    out_specs = (
        P(("wide", "narrow"), None),
        P(("wide", "narrow"), None),
        P(("wide", "narrow"), None),
        P(),
        P(),
        P("wide", "narrow"),
        P("wide", "narrow"),
        P("wide", "narrow"),
        P("narrow", "wide"),
        P("wide", "narrow"),
        P("wide", "narrow"),
        P("wide", "narrow"),
        P("narrow", "wide"),
        P("wide", "narrow"),
        P("narrow", "wide"),
    )
    return jax.shard_map(body, mesh=mesh, in_specs=in_specs, out_specs=out_specs, check_vma=False)
```

```python
import jax
import jax.numpy as jnp
from jax import lax
from jax.sharding import PartitionSpec as P

HEAD_DIM = 128
PIX = 256
CHUNKS = 2

EPSILON = 1e-06
MASKED = -1000000000.0
BF = jnp.bfloat16
F32 = jnp.float32


def product(left_side, right_side):
    return lax.dot_general(
        left_side,
        right_side,
        (((left_side.ndim - 1,), (0,)), ((), ())),
        preferred_element_type=F32,
    )


def right_inner(left_side, right_side):
    return lax.dot_general(
        left_side,
        right_side,
        (((left_side.ndim - 1,), (1,)), ((), ())),
        preferred_element_type=F32,
    )


def left_inner(left_side, right_side):
    rows = tuple(range(left_side.ndim - 1))
    return lax.dot_general(left_side, right_side, ((rows, rows), ((), ())), preferred_element_type=F32)


def follow(value, *others):
    if not others:
        return value
    nothing = sum(o[(0,) * o.ndim].astype(F32) for o in others) * 0.0
    return value + nothing.astype(value.dtype)


def whole(value):
    return lax.optimization_barrier(value)


def after(value, *others):
    return lax.optimization_barrier((value, *others))[0]


def spread(name, rows, gates={}):
    n = lax.axis_size("narrow")
    here = lax.axis_index("narrow")
    with jax.named_scope("spread_" + name):
        up, down = [rows], [rows]
        for step in range(1, n):
            one, other = follow(up[-1], *gates.get(step, ())), follow(down[-1], *gates.get(step, ()))
            up.append(lax.ppermute(one, "narrow", [(k, k + 1) for k in range(step - 1, n - 1)]))
            down.append(lax.ppermute(other, "narrow", [(k, k - 1) for k in range(1, n - step + 1)]))
        parts = [rows] + [jnp.where(here >= s, up[s], down[n - s]) for s in range(1, n)]
        return jnp.stack(parts), [(up[s], down[s]) for s in range(1, n)]


def sink(name, parts, gates={}, hops=(), until=None):
    n = lax.axis_size("narrow")
    hops = list(hops)
    with jax.named_scope("sink_" + name):
        for step in range(len(hops) + 1, until or n):
            one, other = parts[step], parts[n - step]
            if hops:
                one = hops[-1][0].astype(F32) + one.astype(F32)
                other = hops[-1][1].astype(F32) + other.astype(F32)
            one, other = follow(one, *gates.get(step, ())), follow(other, *gates.get(step, ()))
            up = lax.ppermute(one.astype(BF), "narrow", [(k, k + 1) for k in range(step)])
            down = lax.ppermute(other.astype(BF), "narrow", [(k, k - 1) for k in range(n - step, n)])
            hops.append((up, down))
        if until:
            return None, hops
        return up.astype(F32) + down.astype(F32) + parts[0].astype(F32), hops


def norm_stats(features):
    center = features - jnp.mean(features, axis=-1, keepdims=True)
    rstd = lax.rsqrt(jnp.mean(center * center, axis=-1, keepdims=True) + EPSILON)
    return center * rstd, rstd


def norm_back(grad, xhat, rstd, gain):
    scaled = grad * gain
    return rstd * (
        scaled
        - jnp.mean(scaled, axis=-1, keepdims=True)
        - xhat * jnp.mean(scaled * xhat, axis=-1, keepdims=True)
    )


def norm_sums(grad, xhat):
    return jnp.stack([jnp.sum(grad * xhat, axis=0), jnp.sum(grad, axis=0)])


def score_block(queries, keys_in, allowed, score_scale):
    raw = jnp.einsum("iphe,iqhe->ihpq", queries, keys_in, preferred_element_type=F32)
    return jnp.where(allowed[:, None], raw * score_scale, MASKED)


def attend(queries, keys_in, values_in, allowed, score_scale):
    scores = score_block(queries, keys_in, allowed, score_scale)
    log_total = jax.nn.logsumexp(scores, axis=-1, keepdims=True)
    soft = jnp.exp(scores - log_total).astype(BF)
    mixture = jnp.einsum("ihpq,iqhe->iphe", soft, values_in, preferred_element_type=F32)
    return mixture.astype(BF), log_total


def attend_back(queries, keys_in, values_in, allowed, log_total, grad_mix, score_scale):
    soft = jnp.exp(score_block(queries, keys_in, allowed, score_scale) - log_total)
    grad_soft = jnp.einsum("iphe,iqhe->ihpq", grad_mix, values_in, preferred_element_type=F32)
    grad_values = jnp.einsum("ihpq,iphe->iqhe", soft.astype(BF), grad_mix, preferred_element_type=F32)
    row_dot = jnp.sum(soft * grad_soft, axis=-1, keepdims=True)
    grad_scores = whole((soft * (grad_soft - row_dot) * score_scale).astype(BF))
    grad_queries = jnp.einsum("ihpq,iqhe->iphe", grad_scores, keys_in, preferred_element_type=F32)
    grad_keys = jnp.einsum("ihpq,iphe->iqhe", grad_scores, queries, preferred_element_type=F32)
    return grad_queries.astype(BF), grad_keys, grad_values


def body(
    tokens,
    out_grad,
    captions,
    image_blocks,
    caption_owner,
    norm_gains,
    norm_shifts,
    w_query,
    w_key,
    w_value,
    w_out,
    w_cross_query,
    w_cross_key,
    w_cross_value,
    w_cross_out,
    w_up,
    w_down,
):
    scale = HEAD_DIM ** (-0.5)
    n = lax.axis_size("narrow")
    here = lax.axis_index("narrow")
    width = w_query.shape[1]
    heads = width // HEAD_DIM
    part = PIX // CHUNKS
    chunks = [slice(c * part, (c + 1) * part) for c in range(CHUNKS)]
    image_of = (here - jnp.arange(n)) % n

    def rows_of(*pieces):
        return lax.all_gather(
            jnp.concatenate([p.astype(BF) for p in pieces], axis=1), "wide", axis=0, tiled=True
        )

    def columns_of(piece):
        return lax.all_gather(piece.astype(BF), "wide", axis=1, tiled=True)

    def to_rows(g):
        return lax.psum_scatter(g.astype(BF), "wide", scatter_dimension=0, tiled=True).astype(F32)

    def to_columns(g):
        return lax.psum_scatter(g.astype(BF), "wide", scatter_dimension=1, tiled=True).astype(F32)

    full_qkv = rows_of(w_query, w_key, w_value)

    residual0 = tokens.astype(F32)
    xhat1, rstd1 = norm_stats(residual0)
    own1 = (xhat1 * norm_gains[0] + norm_shifts[0]).astype(BF)
    full_out = columns_of(w_out)
    full_ckv = rows_of(w_cross_key, w_cross_value)
    full_cq = rows_of(w_cross_query)
    full_cout = columns_of(w_cross_out)
    full_up = rows_of(w_up)
    full_down = columns_of(w_down)
    normed1 = spread("n1", own1)[0]
    qkv = product(normed1, full_qkv).astype(BF)
    heads_of = lambda x: x.reshape(x.shape[:-1] + (x.shape[-1] // HEAD_DIM, HEAD_DIM))
    self_q, self_k, self_v = [heads_of(qkv[..., k * width : (k + 1) * width]) for k in range(3)]
    blocks = image_blocks[image_of]
    self_allowed = blocks[:, :, None] == blocks[:, None, :]
    self_mix, self_total = attend(self_q, self_k, self_v, self_allowed, scale)
    self_mix = self_mix.reshape(n, PIX, width)

    text = spread("text", follow(captions, normed1[1], normed1[n - 1]), {2: (self_mix,)})[0]
    text_count = text.shape[0] * text.shape[1]
    text_rows = text.reshape(text_count, text.shape[2])
    ckv = product(text_rows, full_ckv).astype(BF)
    cross_k = heads_of(ckv[None, :, :width])
    cross_v = heads_of(ckv[None, :, width:])
    owner = caption_owner[0].reshape(n, -1)[image_of].reshape(-1)
    part_image = jnp.repeat(image_of, part)
    cross_allowed = (part_image[:, None] == owner[None, :])[None]

    state = []
    for c, rows in enumerate(chunks):
        residual1 = residual0[rows] + sink(f"r1_{c}", product(self_mix[:, rows], full_out).astype(BF))[0]
        xhat2, rstd2 = norm_stats(residual1)
        state.append((residual1, xhat2, rstd2))
    normed2 = [
        spread(f"n2_{c}", (s[1] * norm_gains[1] + norm_shifts[1]).astype(BF))[0] for c, s in enumerate(state)
    ]
    grad_all, og_hops = spread("og", follow(out_grad, normed2[0][1], normed2[0][n - 1]))

    cross_q, cross_mix, cross_total, state3 = [], [], [], []
    for c in range(CHUNKS):
        if c > 0:
            normed2[c] = follow(normed2[c], sent, *og_hops[0])
        q = heads_of(product(normed2[c], full_cq).astype(BF).reshape(1, n * part, width))
        mix, total = attend(q, cross_k, cross_v, cross_allowed, scale)
        mix = mix.reshape(n, part, width)
        sent = whole(product(mix, full_cout).astype(BF))
        residual2 = state[c][0] + sink(f"r2_{c}", sent, {1: og_hops[1]} if c > 0 else {})[0]
        xhat3, rstd3 = norm_stats(residual2)
        cross_q.append(q)
        cross_mix.append(mix)
        cross_total.append(total)
        state3.append((residual2, xhat3, rstd3))
    normed3 = [
        spread(f"n3_{c}", (s[1] * norm_gains[2] + norm_shifts[2]).astype(BF))[0] for c, s in enumerate(state3)
    ]

    out_parts, acts, grad_hiddens, grad2, sums3 = [], [], [], [], []
    for c, rows in enumerate(chunks):
        hidden = product(normed3[c], full_up)
        grad_rows = grad_all[:, rows]
        acted, gelu_back = jax.vjp(jax.nn.gelu, hidden)
        acted = acted.astype(BF)
        grad_hidden = gelu_back(right_inner(grad_rows, full_down))[0].astype(BF)
        acts.append(acted)
        grad_hiddens.append(grad_hidden)
        grad_n3 = sink(f"d3_{c}", right_inner(grad_hidden, full_up).astype(BF))[0]
        residual2, xhat3, rstd3 = state3[c]
        sums3.append(norm_sums(grad_n3, xhat3))
        grad2.append(out_grad[rows].astype(F32) + norm_back(grad_n3, xhat3, rstd3, norm_gains[2]))
        out_parts.append(whole(product(acted, full_down).astype(BF)))
    cat = lambda xs: jnp.concatenate(xs, axis=1)
    acted, grad_hidden, n3 = cat(acts), cat(grad_hiddens), cat(normed3)
    grad_down = left_inner(acted, cat([grad_all[:, rows] for rows in chunks]))
    grad_up = left_inner(n3, grad_hidden)

    e2, e2_hops = map(list, zip(*[spread(f"e2_{c}", g.astype(BF)) for c, g in enumerate(grad2)]))
    out_parts = [jnp.concatenate([p[k] for p in out_parts]) for k in range(n)]
    out_hops = sink("out", out_parts, {1: e2_hops[-1][1]}, until=n - 1)[1]
    own_down = to_columns(grad_down)
    own_up = to_rows(grad_up)
    e2[-1] = after(e2[-1], grad_down, grad_up)
    grad1, sums2, grad_cqs, grad_ck, grad_cv = [], [], [], 0.0, 0.0
    for c in range(CHUNKS):
        grad_mix = heads_of(right_inner(e2[c], full_cout).astype(BF).reshape(1, n * part, width))
        gq, gk, gv = attend_back(
            cross_q[c], cross_k, cross_v, cross_allowed, cross_total[c], grad_mix, scale
        )
        gq = gq.reshape(n, part, width)
        grad_cqs.append(gq)
        grad_ck = grad_ck + gk
        grad_cv = grad_cv + gv
        sent = whole(right_inner(gq if c == 0 else follow(gq, *out_hops[0]), full_cq).astype(BF))
        grad_n2 = sink(f"d2_{c}", sent, {1: out_hops[1]} if c > 0 else {})[0]
        _, xhat2, rstd2 = state[c]
        sums2.append(norm_sums(grad_n2, xhat2))
        grad1.append(grad2[c] + norm_back(grad_n2, xhat2, rstd2, norm_gains[1]))
    grad_cout = left_inner(cat(cross_mix), cat(e2))
    grad_cq = left_inner(cat(normed2), cat(grad_cqs))
    grad_ckv = jnp.concatenate(
        [grad_ck.reshape(text_count, width), grad_cv.reshape(text_count, width)], axis=1
    ).astype(BF)
    grad_text_part = whole(right_inner(grad_ckv, full_ckv).astype(BF).reshape(n, -1, text.shape[2]))
    grad_wckv = left_inner(text_rows, grad_ckv)

    e1, e1_hops = map(list, zip(*[spread(f"e1_{c}", g.astype(BF)) for c, g in enumerate(grad1)]))
    own_cout = to_columns(grad_cout)
    own_cq = to_rows(grad_cq)
    own_ckv = to_rows(grad_wckv)
    e1[-1] = after(e1[-1], grad_cout, grad_cq, grad_wckv)
    grad_mix = heads_of(cat([right_inner(e, full_out).astype(BF) for e in e1]))
    grad_mix = after(grad_mix, own_down, own_up)
    gq, gk, gv = attend_back(self_q, self_k, self_v, self_allowed, self_total, grad_mix, scale)
    out_sum, out_hops = sink("out", out_parts, {n - 1: e1_hops[-1][1]}, out_hops)
    block_out = (jnp.concatenate([s[0] for s in state3]) + out_sum).astype(BF)
    grad_text, text_hops = sink("text", grad_text_part, {1: e1_hops[-1][1], 2: (gq,)})
    grad_text = grad_text.astype(BF)
    grad_qkv = jnp.concatenate(
        [g.astype(BF).reshape(n, PIX, width) for g in (gq, gk, gv)], axis=-1
    )
    grad_qkv = follow(grad_qkv, *text_hops[1])
    grad_out = left_inner(self_mix, cat(e1))
    grad_n1_part = whole(right_inner(grad_qkv, full_qkv).astype(BF))
    grad_n1 = sink("d1", grad_n1_part, {1: out_hops[-1]})[0]
    grad_wqkv = left_inner(normed1, after(grad_qkv, grad_n1_part))
    grad1 = jnp.concatenate(grad1)
    grad_n1 = after(grad_n1, own_cout, own_cq, own_ckv)
    grad_tokens = (grad1 + norm_back(grad_n1, xhat1, rstd1, norm_gains[0])).astype(BF)
    sums = lax.psum(
        jnp.stack([norm_sums(grad_n1, xhat1), sum(sums2), sum(sums3)]), ("wide", "narrow")
    )

    own_out = to_columns(grad_out)
    own_qkv = to_rows(grad_wqkv)
    return (
        block_out,
        grad_tokens,
        grad_text,
        sums[:, 0],
        sums[:, 1],
        own_qkv[:, :width],
        own_qkv[:, width : 2 * width],
        own_qkv[:, 2 * width :],
        own_out,
        own_cq,
        own_ckv[:, :width],
        own_ckv[:, width:],
        own_cout,
        own_up,
        own_down,
    )

def solution(mesh):
    in_specs = (
        P(("wide", "narrow"), None),
        P(("wide", "narrow"), None),
        P(("wide", "narrow"), None),
        P("wide", None),
        P("wide", None),
        P(),
        P(),
        P("wide", "narrow"),
        P("wide", "narrow"),
        P("wide", "narrow"),
        P("narrow", "wide"),
        P("wide", "narrow"),
        P("wide", "narrow"),
        P("wide", "narrow"),
        P("narrow", "wide"),
        P("wide", "narrow"),
        P("narrow", "wide"),
    )
    out_specs = (
        P(("wide", "narrow"), None),
        P(("wide", "narrow"), None),
        P(("wide", "narrow"), None),
        P(),
        P(),
        P("wide", "narrow"),
        P("wide", "narrow"),
        P("wide", "narrow"),
        P("narrow", "wide"),
        P("wide", "narrow"),
        P("wide", "narrow"),
        P("wide", "narrow"),
        P("narrow", "wide"),
        P("wide", "narrow"),
        P("narrow", "wide"),
    )
    return jax.shard_map(body, mesh=mesh, in_specs=in_specs, out_specs=out_specs, check_vma=False)
```

```python
import jax
import jax.numpy as jnp
from jax import lax
from jax.sharding import PartitionSpec as P

HEAD_DIM = 128
PIX = 256
CHUNKS = 2

EPSILON = 1e-06
MASKED = -1000000000.0
BF = jnp.bfloat16
F32 = jnp.float32


def product(left_side, right_side):
    return lax.dot_general(
        left_side,
        right_side,
        (((left_side.ndim - 1,), (0,)), ((), ())),
        preferred_element_type=F32,
    )


def right_inner(left_side, right_side):
    return lax.dot_general(
        left_side,
        right_side,
        (((left_side.ndim - 1,), (1,)), ((), ())),
        preferred_element_type=F32,
    )


def left_inner(left_side, right_side):
    rows = tuple(range(left_side.ndim - 1))
    return lax.dot_general(left_side, right_side, ((rows, rows), ((), ())), preferred_element_type=F32)


def follow(value, *others):
    if not others:
        return value
    nothing = sum(o[(0,) * o.ndim].astype(F32) for o in others) * 0.0
    return value + nothing.astype(value.dtype)


def whole(value):
    return lax.optimization_barrier(value)


def after(value, *others):
    return lax.optimization_barrier((value, *others))[0]


def spread(name, rows, gates={}):
    n = lax.axis_size("narrow")
    here = lax.axis_index("narrow")
    with jax.named_scope("spread_" + name):
        up, down = [rows], [rows]
        for step in range(1, n):
            one, other = follow(up[-1], *gates.get(step, ())), follow(down[-1], *gates.get(step, ()))
            up.append(lax.ppermute(one, "narrow", [(k, k + 1) for k in range(step - 1, n - 1)]))
            down.append(lax.ppermute(other, "narrow", [(k, k - 1) for k in range(1, n - step + 1)]))
        parts = [rows] + [jnp.where(here >= s, up[s], down[n - s]) for s in range(1, n)]
        return jnp.stack(parts), [(up[s], down[s]) for s in range(1, n)]


def sink(name, parts, gates={}, hops=(), until=None):
    n = lax.axis_size("narrow")
    hops = list(hops)
    with jax.named_scope("sink_" + name):
        for step in range(len(hops) + 1, until or n):
            one, other = parts[step], parts[n - step]
            if hops:
                one = hops[-1][0].astype(F32) + one.astype(F32)
                other = hops[-1][1].astype(F32) + other.astype(F32)
            one, other = follow(one, *gates.get(step, ())), follow(other, *gates.get(step, ()))
            up = lax.ppermute(one.astype(BF), "narrow", [(k, k + 1) for k in range(step)])
            down = lax.ppermute(other.astype(BF), "narrow", [(k, k - 1) for k in range(n - step, n)])
            hops.append((up, down))
        if until:
            return None, hops
        return up.astype(F32) + down.astype(F32) + parts[0].astype(F32), hops


def norm_stats(features):
    center = features - jnp.mean(features, axis=-1, keepdims=True)
    rstd = lax.rsqrt(jnp.mean(center * center, axis=-1, keepdims=True) + EPSILON)
    return center * rstd, rstd


def norm_back(grad, xhat, rstd, gain):
    scaled = grad * gain
    return rstd * (
        scaled
        - jnp.mean(scaled, axis=-1, keepdims=True)
        - xhat * jnp.mean(scaled * xhat, axis=-1, keepdims=True)
    )


def norm_sums(grad, xhat):
    return jnp.stack([jnp.sum(grad * xhat, axis=0), jnp.sum(grad, axis=0)])


def score_block(queries, keys_in, allowed, score_scale):
    raw = jnp.einsum("iphe,iqhe->ihpq", queries, keys_in, preferred_element_type=F32)
    return jnp.where(allowed[:, None], raw * score_scale, MASKED)


def attend(queries, keys_in, values_in, allowed, score_scale):
    scores = score_block(queries, keys_in, allowed, score_scale)
    log_total = jax.nn.logsumexp(scores, axis=-1, keepdims=True)
    soft = jnp.exp(scores - log_total).astype(BF)
    mixture = jnp.einsum("ihpq,iqhe->iphe", soft, values_in, preferred_element_type=F32)
    return mixture.astype(BF), log_total


def attend_back(queries, keys_in, values_in, allowed, log_total, grad_mix, score_scale):
    soft = jnp.exp(score_block(queries, keys_in, allowed, score_scale) - log_total)
    grad_soft = jnp.einsum("iphe,iqhe->ihpq", grad_mix, values_in, preferred_element_type=F32)
    grad_values = jnp.einsum("ihpq,iphe->iqhe", whole(soft.astype(BF)), grad_mix, preferred_element_type=F32)
    row_dot = jnp.sum(soft * grad_soft, axis=-1, keepdims=True)
    grad_scores = whole((soft * (grad_soft - row_dot) * score_scale).astype(BF))
    grad_queries = jnp.einsum("ihpq,iqhe->iphe", grad_scores, keys_in, preferred_element_type=F32)
    grad_keys = jnp.einsum("ihpq,iphe->iqhe", grad_scores, queries, preferred_element_type=F32)
    return grad_queries.astype(BF), grad_keys, grad_values


def body(
    tokens,
    out_grad,
    captions,
    image_blocks,
    caption_owner,
    norm_gains,
    norm_shifts,
    w_query,
    w_key,
    w_value,
    w_out,
    w_cross_query,
    w_cross_key,
    w_cross_value,
    w_cross_out,
    w_up,
    w_down,
):
    scale = HEAD_DIM ** (-0.5)
    n = lax.axis_size("narrow")
    here = lax.axis_index("narrow")
    width = w_query.shape[1]
    heads = width // HEAD_DIM
    part = PIX // CHUNKS
    chunks = [slice(c * part, (c + 1) * part) for c in range(CHUNKS)]
    image_of = (here - jnp.arange(n)) % n

    def rows_of(*pieces):
        return lax.all_gather(
            jnp.concatenate([p.astype(BF) for p in pieces], axis=1), "wide", axis=0, tiled=True
        )

    def columns_of(piece):
        return lax.all_gather(piece.astype(BF), "wide", axis=1, tiled=True)

    def to_rows(g):
        return lax.psum_scatter(g.astype(BF), "wide", scatter_dimension=0, tiled=True).astype(F32)

    def to_columns(g):
        return lax.psum_scatter(g.astype(BF), "wide", scatter_dimension=1, tiled=True).astype(F32)

    full_qkv = rows_of(w_query, w_key, w_value)

    residual0 = tokens.astype(F32)
    xhat1, rstd1 = norm_stats(residual0)
    own1 = (xhat1 * norm_gains[0] + norm_shifts[0]).astype(BF)
    full_out = columns_of(w_out)
    full_ckv = rows_of(w_cross_key, w_cross_value)
    full_cq = rows_of(w_cross_query)
    full_cout = columns_of(w_cross_out)
    full_up = rows_of(w_up)
    full_down = columns_of(w_down)
    normed1 = spread("n1", own1)[0]
    qkv = product(normed1, full_qkv).astype(BF)
    heads_of = lambda x: x.reshape(x.shape[:-1] + (x.shape[-1] // HEAD_DIM, HEAD_DIM))
    self_q, self_k, self_v = [heads_of(qkv[..., k * width : (k + 1) * width]) for k in range(3)]
    blocks = image_blocks[image_of]
    self_allowed = blocks[:, :, None] == blocks[:, None, :]
    self_mix, self_total = attend(self_q, self_k, self_v, self_allowed, scale)
    self_mix = self_mix.reshape(n, PIX, width)

    text = spread("text", follow(captions, normed1[1], normed1[n - 1]), {2: (self_mix,)})[0]
    text_count = text.shape[0] * text.shape[1]
    text_rows = text.reshape(text_count, text.shape[2])
    ckv = product(text_rows, full_ckv).astype(BF)
    cross_k = heads_of(ckv[None, :, :width])
    cross_v = heads_of(ckv[None, :, width:])
    owner = caption_owner[0].reshape(n, -1)[image_of].reshape(-1)
    part_image = jnp.repeat(image_of, part)
    cross_allowed = (part_image[:, None] == owner[None, :])[None]

    state = []
    for c, rows in enumerate(chunks):
        residual1 = residual0[rows] + sink(f"r1_{c}", product(self_mix[:, rows], full_out).astype(BF))[0]
        xhat2, rstd2 = norm_stats(residual1)
        state.append((residual1, xhat2, rstd2))
    normed2 = [
        spread(f"n2_{c}", (s[1] * norm_gains[1] + norm_shifts[1]).astype(BF))[0] for c, s in enumerate(state)
    ]
    grad_all, og_hops = spread("og", follow(out_grad, normed2[0][1], normed2[0][n - 1]))

    cross_q, cross_mix, cross_total, state3 = [], [], [], []
    for c in range(CHUNKS):
        if c > 0:
            normed2[c] = follow(normed2[c], sent, *og_hops[0])
        q = heads_of(product(normed2[c], full_cq).astype(BF).reshape(1, n * part, width))
        mix, total = attend(q, cross_k, cross_v, cross_allowed, scale)
        mix = mix.reshape(n, part, width)
        sent = whole(product(mix, full_cout).astype(BF))
        residual2 = state[c][0] + sink(f"r2_{c}", sent, {1: og_hops[1]} if c > 0 else {})[0]
        xhat3, rstd3 = norm_stats(residual2)
        cross_q.append(q)
        cross_mix.append(mix)
        cross_total.append(total)
        state3.append((residual2, xhat3, rstd3))
    normed3 = [
        spread(f"n3_{c}", (s[1] * norm_gains[2] + norm_shifts[2]).astype(BF))[0] for c, s in enumerate(state3)
    ]

    out_parts, acts, grad_hiddens, grad2, sums3 = [], [], [], [], []
    for c, rows in enumerate(chunks):
        hidden = product(normed3[c], full_up)
        grad_rows = grad_all[:, rows]
        acted, gelu_back = jax.vjp(jax.nn.gelu, hidden)
        acted = acted.astype(BF)
        grad_hidden = gelu_back(right_inner(grad_rows, full_down))[0].astype(BF)
        acts.append(acted)
        grad_hiddens.append(grad_hidden)
        grad_n3 = sink(f"d3_{c}", right_inner(grad_hidden, full_up).astype(BF))[0]
        residual2, xhat3, rstd3 = state3[c]
        sums3.append(norm_sums(grad_n3, xhat3))
        grad2.append(out_grad[rows].astype(F32) + norm_back(grad_n3, xhat3, rstd3, norm_gains[2]))
        out_parts.append(whole(product(acted, full_down).astype(BF)))
    cat = lambda xs: jnp.concatenate(xs, axis=1)
    acted, grad_hidden, n3 = cat(acts), cat(grad_hiddens), cat(normed3)
    grad_down = left_inner(acted, cat([grad_all[:, rows] for rows in chunks]))
    grad_up = left_inner(n3, grad_hidden)

    e2, e2_hops = map(list, zip(*[spread(f"e2_{c}", g.astype(BF)) for c, g in enumerate(grad2)]))
    out_parts = [jnp.concatenate([p[k] for p in out_parts]) for k in range(n)]
    out_hops = sink("out", out_parts, {1: e2_hops[-1][1]}, until=n - 1)[1]
    own_down = to_columns(grad_down)
    own_up = to_rows(grad_up)
    e2[-1] = after(e2[-1], grad_down, grad_up)
    grad1, sums2, grad_cqs, grad_ck, grad_cv = [], [], [], 0.0, 0.0
    for c in range(CHUNKS):
        grad_mix = heads_of(right_inner(e2[c], full_cout).astype(BF).reshape(1, n * part, width))
        gq, gk, gv = attend_back(
            cross_q[c], cross_k, cross_v, cross_allowed, cross_total[c], grad_mix, scale
        )
        gq = gq.reshape(n, part, width)
        grad_cqs.append(gq)
        grad_ck = grad_ck + gk
        grad_cv = grad_cv + gv
        sent = whole(right_inner(gq if c == 0 else follow(gq, *out_hops[0]), full_cq).astype(BF))
        grad_n2 = sink(f"d2_{c}", sent, {1: out_hops[1]} if c > 0 else {})[0]
        _, xhat2, rstd2 = state[c]
        sums2.append(norm_sums(grad_n2, xhat2))
        grad1.append(grad2[c] + norm_back(grad_n2, xhat2, rstd2, norm_gains[1]))
    grad_cout = left_inner(cat(cross_mix), cat(e2))
    grad_cq = left_inner(cat(normed2), cat(grad_cqs))
    grad_ckv = jnp.concatenate(
        [grad_ck.reshape(text_count, width), grad_cv.reshape(text_count, width)], axis=1
    ).astype(BF)
    grad_text_part = whole(right_inner(grad_ckv, full_ckv).astype(BF).reshape(n, -1, text.shape[2]))
    grad_wckv = left_inner(text_rows, grad_ckv)

    e1, e1_hops = map(list, zip(*[spread(f"e1_{c}", g.astype(BF)) for c, g in enumerate(grad1)]))
    own_cout = to_columns(grad_cout)
    own_cq = to_rows(grad_cq)
    own_ckv = to_rows(grad_wckv)
    e1[-1] = after(e1[-1], grad_cout, grad_cq, grad_wckv)
    grad_mix = heads_of(cat([right_inner(e, full_out).astype(BF) for e in e1]))
    grad_mix = after(grad_mix, own_down, own_up)
    gq, gk, gv = attend_back(self_q, self_k, self_v, self_allowed, self_total, grad_mix, scale)
    out_sum, out_hops = sink("out", out_parts, {n - 1: e1_hops[-1][1]}, out_hops)
    block_out = (jnp.concatenate([s[0] for s in state3]) + out_sum).astype(BF)
    grad_text, text_hops = sink("text", grad_text_part, {1: e1_hops[-1][1], 2: (gq,)})
    grad_text = grad_text.astype(BF)
    grad_qkv = jnp.concatenate(
        [g.astype(BF).reshape(n, PIX, width) for g in (gq, gk, gv)], axis=-1
    )
    grad_qkv = follow(grad_qkv, *text_hops[1])
    grad_out = left_inner(self_mix, cat(e1))
    grad_n1_part = whole(right_inner(grad_qkv, full_qkv).astype(BF))
    grad_n1 = sink("d1", grad_n1_part, {1: out_hops[-1]})[0]
    grad_wqkv = left_inner(normed1, after(grad_qkv, grad_n1_part))
    grad1 = jnp.concatenate(grad1)
    grad_n1 = after(grad_n1, own_cout, own_cq, own_ckv)
    grad_tokens = (grad1 + norm_back(grad_n1, xhat1, rstd1, norm_gains[0])).astype(BF)
    sums = lax.psum(
        jnp.stack([norm_sums(grad_n1, xhat1), sum(sums2), sum(sums3)]), ("wide", "narrow")
    )

    own_out = to_columns(grad_out)
    own_qkv = to_rows(grad_wqkv)
    return (
        block_out,
        grad_tokens,
        grad_text,
        sums[:, 0],
        sums[:, 1],
        own_qkv[:, :width],
        own_qkv[:, width : 2 * width],
        own_qkv[:, 2 * width :],
        own_out,
        own_cq,
        own_ckv[:, :width],
        own_ckv[:, width:],
        own_cout,
        own_up,
        own_down,
    )

def solution(mesh):
    in_specs = (
        P(("wide", "narrow"), None),
        P(("wide", "narrow"), None),
        P(("wide", "narrow"), None),
        P("wide", None),
        P("wide", None),
        P(),
        P(),
        P("wide", "narrow"),
        P("wide", "narrow"),
        P("wide", "narrow"),
        P("narrow", "wide"),
        P("wide", "narrow"),
        P("wide", "narrow"),
        P("wide", "narrow"),
        P("narrow", "wide"),
        P("wide", "narrow"),
        P("narrow", "wide"),
    )
    out_specs = (
        P(("wide", "narrow"), None),
        P(("wide", "narrow"), None),
        P(("wide", "narrow"), None),
        P(),
        P(),
        P("wide", "narrow"),
        P("wide", "narrow"),
        P("wide", "narrow"),
        P("narrow", "wide"),
        P("wide", "narrow"),
        P("wide", "narrow"),
        P("wide", "narrow"),
        P("narrow", "wide"),
        P("wide", "narrow"),
        P("narrow", "wide"),
    )
    return jax.shard_map(body, mesh=mesh, in_specs=in_specs, out_specs=out_specs, check_vma=False)
```
